512 devices in a mesh: depth: 16 (over z, y_lo), rows: 32 (over x, y_hi, core).
Axes of the slice: x: 4, y: 8 (y_hi: 4, y_lo: 2; y = y_hi * 2 + y_lo), z: 8, core: 2. Of those that a mesh axis runs over, the one named last changes fastest.
Arguments:
- target: float32 [16, 2, 4096, 4096], P('depth', None, 'rows'), may hold values from -6 to 6
- depth_index: int32 [16], P('depth'), may hold values from 0 to 255
- band_mask: int32 [16, 2, 4096], P('depth'), may hold values from 0 to 1, as said below
Outputs:
- hologram: float32 [2, 4096, 4096], P(None, ('depth', 'rows'))
The draws below stay inside these ranges and needn't reach their ends.
Inputs may be any that keep to these rules, and one draw needn't show every extreme that they name: `band_mask`: for each plane and each of the two dimensions, the ones are exactly the frequency indices k with min(k, 4096 - k) below a cutoff between 512 and 2048.
All inputs are finite; a program needn't handle non-finite values.
Results may differ from the reference program's by a relative error of at most 0.0009.
Values sent between devices are 32-bit elements; how exact they have to be, the bound alone decides.
A program may use at most 64 MiB of HBM per device.

```python
import math
import jax
import jax.numpy as jnp
from jax import lax

N = 4096
PLANES = 16
DEPTHS = 256


def draw_band_mask(key, part):
    cutoff = jax.random.randint(key, (PLANES, 2, 1), N // 8, N // 2 + 1)
    indices = jnp.arange(N, dtype=jnp.int32)
    folded = jnp.minimum(indices, N - indices)
    return (folded[None, None, :] < cutoff).astype(jnp.int32)


def place_ends(values, key, low, top_value):
    spot = [jax.random.randint(jax.random.fold_in(key, axis), (), 0, length) for axis, length in enumerate(values.shape)]
    main_axis = values.shape.index(max(values.shape))
    neighbour = spot[:main_axis] + [(spot[main_axis] + 1) % values.shape[main_axis]] + spot[main_axis + 1:]
    return values.at[tuple(spot)].set(low).at[tuple(neighbour)].set(top_value)


def levels(stream_key, dims, cuts, low, top_value):
    loudness = 1.0
    for axis_at, parts in cuts:
        steps = jax.random.uniform(jax.random.fold_in(jax.random.fold_in(stream_key, 6), axis_at), (parts,), jnp.float32, low / len(cuts), top_value / len(cuts))
        loudness = loudness * jnp.repeat(jnp.exp(steps), dims[axis_at] // parts).reshape((-1,) + (1,) * (len(dims) - 1 - axis_at))
    return loudness


def normal_values(key, dims, width, reach, split=(), kind=jnp.bfloat16):
    result = jax.random.normal(key, dims, jnp.float32) * width
    if len(split) > 0:
        result = levels(key, dims, split, -0.22, 0.18) * result
    return jnp.clip(result, min=-reach, max=reach).astype(kind)


def setup_inputs(seed: int = 0) -> dict:
    key_of = jax.random.split(jax.random.key(seed), 4)
    return {
        "target": normal_values(key_of[0], (PLANES, 2, N, N), 1.0, 6.0, ((0, 16), (2, 32)), jnp.float32),
        "depth_index": place_ends(jax.random.randint(key_of[1], (PLANES,), 0, DEPTHS), jax.random.fold_in(key_of[1], 1), 0, DEPTHS - 1).astype(jnp.int32),
        "band_mask": draw_band_mask(jax.random.fold_in(key_of[3], 71), 0),
    }


def reference(target, depth_index, band_mask):
    planes_all = target.shape[0]
    indices = jnp.arange(N, dtype=jnp.int32)
    signed = jnp.where(indices < N // 2, indices, indices - N)
    frequency = signed.astype(jnp.float32) / N
    radical = jnp.sqrt(4.0 - frequency[:, None] ** 2 - frequency[None, :] ** 2)

    def add_plane(running_sum, inputs):
        plane_data, level_index, mask_pair = inputs
        wavefront = lax.complex(plane_data[0], plane_data[1])
        spectrum = jnp.fft.fft2(wavefront, norm='ortho')
        distance = 100.0 + 2.0 * level_index.astype(jnp.float32)
        phases = 2.0 * math.pi * distance * (radical - 2.0)
        weights = mask_pair[0].astype(jnp.float32)[:, None] * mask_pair[1].astype(jnp.float32)[None, :]
        rotated = spectrum * lax.complex(jnp.cos(phases) * weights, jnp.sin(phases) * weights)
        return (running_sum + rotated, None)
    zeros_real = jnp.zeros((N, N), dtype=jnp.float32)
    initial = lax.complex(zeros_real, zeros_real)
    summed, _ = lax.scan(add_plane, initial, (target, depth_index, band_mask))
    field_out = jnp.fft.ifft2(summed, norm='ortho') / jnp.sqrt(jnp.float32(planes_all))
    return jnp.stack([jnp.real(field_out), jnp.imag(field_out)]).astype(jnp.float32)
```

```python
import functools
import math

import jax
import jax.numpy as jnp
import ml_dtypes
import numpy as np
from jax import lax
from jax.experimental import pallas as pl
from jax.experimental.pallas import tpu as pltpu
from jax.sharding import PartitionSpec as P

MESH = pl.DeviceIdType.MESH
N = 4096
LOW = 32
HIGH = 128
Z = 8
CHUNKS = 4
CW = HIGH // CHUNKS
CT = CW // 8
F32 = jnp.float32
BF16 = jnp.bfloat16


def tables():
    angle = 2.0 * np.pi / N * np.outer(np.arange(LOW), np.arange(HIGH))
    turn = np.stack([np.cos(angle), np.sin(angle)]) / 64.0
    turn = np.broadcast_to(turn[:, :, None, :], (2, LOW, 8, HIGH)).astype(np.float32)
    angle = 2.0 * np.pi / LOW * np.outer(np.arange(1, 4), np.arange(8))
    small = np.stack([np.cos(angle), np.sin(angle)])
    small = np.broadcast_to(small[:, :, :, None, None], (2, 3, 8, 8, HIGH)).astype(np.float32)
    angle = 2.0 * np.pi / HIGH * (np.outer(np.arange(HIGH), np.arange(HIGH)) % HIGH)
    cosine, sine = np.cos(angle), np.sin(angle)
    ahead = np.block([[cosine, -sine], [sine, cosine]])
    parts = []
    for matrix in (ahead, ahead.T):
        top = matrix.astype(np.float32).astype(ml_dtypes.bfloat16)
        rest = (matrix - top.astype(np.float64)).astype(np.float32).astype(ml_dtypes.bfloat16)
        parts += [top, rest]
    return turn, small, np.stack(parts)


def dft4(a, sign):
    (r0, i0), (r1, i1), (r2, i2), (r3, i3) = a
    s0r, s0i, d0r, d0i = r0 + r2, i0 + i2, r0 - r2, i0 - i2
    s1r, s1i, d1r, d1i = r1 + r3, i1 + i3, r1 - r3, i1 - i3
    up, down = (d0r - d1i, d0i + d1r), (d0r + d1i, d0i - d1r)
    first, third = (up, down) if sign > 0 else (down, up)
    return [(s0r + s1r, s0i + s1i), first, (s0r - s1r, s0i - s1i), third]


def dft32(re, im, small_ref, sign):
    half = math.sqrt(0.5)
    columns = dft4([(re[8 * n : 8 * n + 8], im[8 * n : 8 * n + 8]) for n in range(4)], sign)
    turned = [columns[0]]
    for k in range(1, 4):
        r, i = columns[k]
        c, s = small_ref[0, k - 1], small_ref[1, k - 1]
        turned.append((r * c + i * s, i * c - r * s) if sign < 0 else (r * c - i * s, i * c + r * s))
    re = jnp.stack([t[0] for t in turned])
    im = jnp.stack([t[1] for t in turned])
    rows = [(re[:, n], im[:, n]) for n in range(8)]
    even = dft4(rows[0::2], sign)
    odd = dft4(rows[1::2], sign)
    (r1, i1), (r2, i2), (r3, i3) = odd[1:]
    if sign < 0:
        odd = [odd[0], ((r1 + i1) * half, (i1 - r1) * half), (i2, -r2), ((i3 - r3) * half, (-r3 - i3) * half)]
    else:
        odd = [odd[0], ((r1 - i1) * half, (i1 + r1) * half), (-i2, r2), ((-r3 - i3) * half, (r3 - i3) * half)]
    result = [(e[0] + o[0], e[1] + o[1]) for e, o in zip(even, odd)]
    return result + [(e[0] - o[0], e[1] - o[1]) for e, o in zip(even, odd)]


def joined(pieces):
    return jnp.concatenate([p[0] for p in pieces]), jnp.concatenate([p[1] for p in pieces])


def split_dot(left, w_ref, which):
    top = left.astype(BF16)
    rest = (left - top.astype(F32)).astype(BF16)
    w_top, w_rest = w_ref[which], w_ref[which + 1]
    dot = functools.partial(jnp.dot, preferred_element_type=F32)
    return dot(top, w_top) + (dot(rest, w_top) + dot(top, w_rest))


def along_lanes(re, im, w_ref, which):
    left = jnp.concatenate([re.reshape(8 * LOW, HIGH), im.reshape(8 * LOW, HIGH)], axis=1)
    result = split_dot(left, w_ref, which)
    return result[:, :HIGH].reshape(LOW, 8, HIGH), result[:, HIGH:].reshape(LOW, 8, HIGH)


def kernel(
    x_ref, mask_ref, level_ref, turn_ref, small_ref, w_ref, out_ref,
    xbuf, tbuf, send, recv, prop, part, ring, own, pair, final, final_in, mask_in, level_in,
    x_sem, send_sem, recv_sem, ring_send, ring_recv, pair_send, pair_recv, final_send, final_recv, par_send, par_recv,
):
    depth = lax.axis_index("depth")
    row = lax.axis_index("rows")
    z, y_lo = depth // 2, lax.rem(depth, 2)
    core, y_hi, x = lax.rem(row, 2), lax.rem(row // 2, 4), row // 8
    other = depth + 1 - 2 * y_lo
    up, down = lax.rem(depth + 2, 2 * Z), lax.rem(depth + 2 * Z - 2, 2 * Z)

    def peer(i):
        h = lax.rem(i, 4)
        to_y = lax.rem(y_hi + lax.rem(h, 2) * 2 + h // 2, 4)
        to_core = lax.rem(core + lax.rem(i // 4, 2), 2)
        to_x = lax.rem(x + i // 8, 4)
        return (to_x * 4 + to_y) * 2 + to_core

    def load(a):
        return pltpu.make_async_copy(x_ref.at[0, :, :, pl.ds(pl.multiple_of(a * HIGH, HIGH), HIGH)], xbuf.at[a], x_sem)

    lax.fori_loop(0, LOW, lambda a, c: (load(a).start(), c)[1], 0)

    barrier = pltpu.get_barrier_semaphore()

    def greet(i, c):
        pl.semaphore_signal(barrier, inc=1, device_id=(other, i), device_id_type=MESH)
        return c

    lax.fori_loop(0, 32, greet, 0)
    pl.semaphore_signal(barrier, inc=1, device_id=(up, row), device_id_type=MESH)
    pl.semaphore_signal(barrier, inc=1, device_id=(down, row), device_id_type=MESH)

    pltpu.make_async_copy(xbuf, xbuf, x_sem).wait()

    def width_first(t, c):
        rows = pl.ds(pl.multiple_of(t * 8, 8), 8)
        re, im = joined(dft32(xbuf[:, 0, rows, :], xbuf[:, 1, rows, :], small_ref, -1))
        cosine, sine = turn_ref[0], turn_ref[1]
        tbuf[:, 0, rows, :] = re * cosine + im * sine
        tbuf[:, 1, rows, :] = im * cosine - re * sine
        return c

    lax.fori_loop(0, 16, width_first, 0)

    pl.semaphore_wait(barrier, 34)

    mask_copy = pltpu.make_async_remote_copy(
        mask_ref, mask_in, par_send.at[0], par_recv.at[0], device_id=(other, row), device_id_type=MESH
    )
    level_copy = pltpu.make_async_remote_copy(
        level_ref, level_in, par_send.at[1], par_recv.at[1], device_id=(other, row), device_id_type=MESH
    )
    mask_copy.start()
    level_copy.start()

    def exchange(q, to):
        return pltpu.make_async_remote_copy(
            send.at[q, to], recv.at[q, row], send_sem.at[q], recv_sem.at[q], device_id=(other, to), device_id_type=MESH
        )

    def exchange_whole(q):
        return pltpu.make_async_remote_copy(
            send.at[q], recv.at[q], send_sem.at[q], recv_sem.at[q], device_id=(other, row), device_id_type=MESH
        )

    def width_last(g, c):
        @pl.when(g > 0)
        def _():
            for h in range(4):
                exchange(0, peer((g - 1) * 4 + h)).start()

        for h in range(4):
            to = peer(g * 4 + h)
            both = split_dot(jnp.concatenate([tbuf[to, 0], tbuf[to, 1]], axis=1), w_ref, 0)
            for k in range(2):
                turned = both[:, k * HIGH : (k + 1) * HIGH].T
                for q in range(CHUNKS):
                    send[q, to, k] = turned[q * CW : (q + 1) * CW]
        return c

    lax.fori_loop(0, 8, width_last, 0)
    lax.fori_loop(28, 32, lambda i, c: (exchange(0, peer(i)).start(), c)[1], 0)
    lax.fori_loop(0, 32, lambda i, c: (exchange(1, peer(i)).start(), c)[1], 0)

    mask_copy.wait()
    level_copy.wait()
    distance = 100.0 + 2.0 * level_in[...].astype(F32)

    def cutoff(k):
        total = jnp.sum(jnp.sum(mask_in[k].astype(F32), axis=1, keepdims=True), axis=0, keepdims=True)
        return jnp.broadcast_to((total + 1.0) * 0.5, (8, HIGH))[None]

    cut_y, cut_x = cutoff(0), cutoff(1)
    shape = (8, 8, HIGH)

    def signed(k):
        return jnp.where(k < N // 2, k, k - N).astype(F32)

    def propagate(i, c):
        t, g = i // 4, lax.rem(i, 4)
        k_y = signed(lax.broadcasted_iota(jnp.int32, shape, 0) + g * 8 + 32 * lax.broadcasted_iota(jnp.int32, shape, 2))
        k_x = signed(row + 32 * (t * 8 + lax.broadcasted_iota(jnp.int32, shape, 1)))
        f_y, f_x = k_y * (1.0 / N), k_x * (1.0 / N)
        square = f_y * f_y + f_x * f_x
        quarters = (-4.0 * distance[None]) * (square / (2.0 + jnp.sqrt(4.0 - square)))
        whole = jnp.floor(quarters + 0.5)
        v = (quarters - whole) * (0.5 * math.pi)
        quadrant = whole - 4.0 * jnp.floor(whole * 0.25)
        v2 = v * v
        sine = v + v * v2 * (-1.6666654611e-1 + v2 * (8.3321608736e-3 - v2 * 1.9515295891e-4))
        cosine = 1.0 - 0.5 * v2 + v2 * v2 * (4.166664568298827e-2 + v2 * (-1.388731625493765e-3 + v2 * 2.443315711809948e-5))
        odd = (quadrant == 1.0) | (quadrant == 3.0)
        re = jnp.where(odd, sine, cosine)
        im = jnp.where(odd, cosine, sine)
        inside = (jnp.abs(k_y) < cut_y) & (jnp.abs(k_x) < cut_x)
        weight = jnp.where(inside, 1.0, 0.0)
        prop[t, pl.ds(g * 8, 8), 0] = jnp.where((quadrant == 1.0) | (quadrant == 2.0), -re, re) * weight
        prop[t, pl.ds(g * 8, 8), 1] = jnp.where(quadrant >= 2.0, -im, im) * weight
        return c

    lax.fori_loop(0, 64, propagate, 0)

    def ring_copy(q, step, toward, source):
        return pltpu.make_async_remote_copy(
            part.at[q, pl.ds(source * 4, 4)], ring.at[q, step], ring_send.at[q, step], ring_recv.at[q, step],
            device_id=(toward, row), device_id_type=MESH,
        )

    def pair_copy(q):
        return pltpu.make_async_remote_copy(
            own.at[q, pl.ds(y_lo * 2, 2)], pair.at[q], pair_send.at[q], pair_recv.at[q],
            device_id=(other, row), device_id_type=MESH,
        )

    def chunk(q, c):
        exchange_whole(q).wait_recv()

        def tile(t, c):
            rows = pl.ds(pl.multiple_of(t * 8, 8), 8)
            re, im = joined(dft32(recv[q, :, 0, rows, :], recv[q, :, 1, rows, :], small_ref, -1))
            cosine, sine = turn_ref[0], turn_ref[1]
            re, im = along_lanes(re * cosine + im * sine, im * cosine - re * sine, w_ref, 0)
            p_re, p_im = prop[q * CT + t, :, 0], prop[q * CT + t, :, 1]
            re, im = along_lanes(re * p_re - im * p_im, re * p_im + im * p_re, w_ref, 2)
            re, im = joined(dft32(re * cosine - im * sine, im * cosine + re * sine, small_ref, 1))
            part[q, :, 0, rows, :] = re
            part[q, :, 1, rows, :] = im
            return c

        lax.fori_loop(0, CT, tile, 0)

        @pl.when(q < CHUNKS - 2)
        def _():
            lax.fori_loop(0, 32, lambda i, c: (exchange(q + 2, peer(i)).start(), c)[1], 0)

        ring_copy(q, 0, up, lax.rem(z + 4, Z)).start()
        ring_copy(q, 4, down, lax.rem(z + 5, Z)).start()
        for step in range(1, 4):
            source = lax.rem(z + 4 - step, Z)
            ring_copy(q, step - 1, up, source).wait_recv()
            part[q, pl.ds(source * 4, 4)] = part[q, pl.ds(source * 4, 4)] + ring[q, step - 1]
            if step < 3:
                back = lax.rem(z + 5 + step, Z)
                ring_copy(q, 3 + step, down, back).wait_recv()
                part[q, pl.ds(back * 4, 4)] = part[q, pl.ds(back * 4, 4)] + ring[q, 3 + step]
            ring_copy(q, step, up, source).start()
            if step < 3:
                ring_copy(q, 4 + step, down, back).start()
        ring_copy(q, 6, down, z).wait_recv()
        ring_copy(q, 3, up, z).wait_recv()
        own[q] = part[q, pl.ds(z * 4, 4)] + (ring[q, 3] + ring[q, 6])
        pair_copy(q).start()
        return c

    lax.fori_loop(0, CHUNKS, chunk, 0)

    for q in range(CHUNKS):
        pair_copy(q).wait_recv()
    keep = 2 - 2 * y_lo
    for half in range(2):
        for k in range(2):
            block = jnp.concatenate([own[q, keep + half, k] + pair[q, half, k] for q in range(CHUNKS)])
            final[half * 16 : half * 16 + 16, k] = block.T.reshape(16, 8, HIGH)

    def deliver(to):
        return pltpu.make_async_remote_copy(
            final.at[to], final_in.at[row], final_send, final_recv, device_id=(other, to), device_id_type=MESH
        )

    deliver_whole = pltpu.make_async_remote_copy(
        final, final_in, final_send, final_recv, device_id=(other, row), device_id_type=MESH
    )
    lax.fori_loop(0, 32, lambda i, c: (deliver(peer(i)).start(), c)[1], 0)

    def settle(q, c):
        exchange_whole(q).wait_send()
        pair_copy(q).wait_send()
        for step in range(7):
            ring_copy(q, step, up, z).wait_send()
        return c

    lax.fori_loop(0, CHUNKS, settle, 0)
    deliver_whole.wait_recv()

    re, im = along_lanes(final_in[:, 0], final_in[:, 1], w_ref, 2)
    cosine, sine = turn_ref[0] * 0.25, turn_ref[1] * 0.25
    pieces = dft32(re * cosine - im * sine, im * cosine + re * sine, small_ref, 1)
    for k in range(8):
        for j in range(4):
            lanes = pl.ds((k * 4 + j) * HIGH, HIGH)
            out_ref[0, :, lanes] = pieces[k][0][j]
            out_ref[1, :, lanes] = pieces[k][1][j]
    deliver_whole.wait_send()


def local(target, depth_index, band_mask):
    turn, small, matrices = tables()
    level = jnp.broadcast_to(depth_index.reshape(1, 1), (8, HIGH))
    vmem = pl.BlockSpec(memory_space=pltpu.VMEM)
    dma = pltpu.SemaphoreType.DMA
    return pl.pallas_call(
        kernel,
        out_shape=jax.ShapeDtypeStruct((2, 8, N), F32),
        in_specs=[pl.BlockSpec(memory_space=pl.ANY)] + [vmem] * 5,
        out_specs=vmem,
        scratch_shapes=[
            pltpu.VMEM((LOW, 2, HIGH, HIGH), F32),
            pltpu.VMEM((LOW, 2, HIGH, HIGH), F32),
            pltpu.VMEM((CHUNKS, LOW, 2, CW, HIGH), F32),
            pltpu.VMEM((CHUNKS, LOW, 2, CW, HIGH), F32),
            pltpu.VMEM((16, LOW, 2, 8, HIGH), F32),
            pltpu.VMEM((CHUNKS, LOW, 2, CW, HIGH), F32),
            pltpu.VMEM((CHUNKS, 7, 4, 2, CW, HIGH), F32),
            pltpu.VMEM((CHUNKS, 4, 2, CW, HIGH), F32),
            pltpu.VMEM((CHUNKS, 2, 2, CW, HIGH), F32),
            pltpu.VMEM((LOW, 2, 8, HIGH), F32),
            pltpu.VMEM((LOW, 2, 8, HIGH), F32),
            pltpu.VMEM((2, LOW, HIGH), jnp.int32),
            pltpu.VMEM((8, HIGH), jnp.int32),
            dma,
            dma((CHUNKS,)),
            dma((CHUNKS,)),
            dma((CHUNKS, 7)),
            dma((CHUNKS, 7)),
            dma((CHUNKS,)),
            dma((CHUNKS,)),
            dma,
            dma,
            dma((2,)),
            dma((2,)),
        ],
        compiler_params=pltpu.CompilerParams(
            collective_id=0, has_side_effects=True, vmem_limit_bytes=60 * 1024 * 1024
        ),
        name="hologram",
    )(target, band_mask.reshape(2, LOW, HIGH), level, turn, small, matrices)


def solution(mesh):
    in_specs = (P("depth", None, "rows", None), P("depth"), P("depth", None, None))
    out_specs = P(None, ("depth", "rows"), None)
    return jax.shard_map(local, mesh=mesh, in_specs=in_specs, out_specs=out_specs, check_vma=False)
```

```python
import functools
import math

import jax
import jax.numpy as jnp
import ml_dtypes
import numpy as np
from jax import lax
from jax.experimental import pallas as pl
from jax.experimental.pallas import tpu as pltpu
from jax.sharding import PartitionSpec as P

MESH = pl.DeviceIdType.MESH
N = 4096
LOW = 32
HIGH = 128
Z = 8
TILES = 16
WIDE = 7
CHUNKS = WIDE + 2
F32 = jnp.float32
BF16 = jnp.bfloat16


def tables():
    angle = 2.0 * np.pi / N * np.outer(np.arange(LOW), np.arange(HIGH))
    turn = np.stack([np.cos(angle), np.sin(angle)]) / 64.0
    turn = np.broadcast_to(turn[:, :, None, :], (2, LOW, 8, HIGH)).astype(np.float32)
    angle = 2.0 * np.pi / LOW * np.outer(np.arange(1, 4), np.arange(8))
    small = np.stack([np.cos(angle), np.sin(angle)])
    small = np.broadcast_to(small[:, :, :, None, None], (2, 3, 8, 8, HIGH)).astype(np.float32)
    angle = 2.0 * np.pi / HIGH * (np.outer(np.arange(HIGH), np.arange(HIGH)) % HIGH)
    cosine, sine = np.cos(angle), np.sin(angle)
    ahead = np.block([[cosine, -sine], [sine, cosine]])
    parts = []
    for matrix in (ahead, ahead.T):
        top = matrix.astype(np.float32).astype(ml_dtypes.bfloat16)
        rest = (matrix - top.astype(np.float64)).astype(np.float32).astype(ml_dtypes.bfloat16)
        parts += [top, rest]
    order = np.arange(256).reshape(2, 2, 64).swapaxes(0, 1).reshape(256)
    parts += [parts[2][order], parts[3][order]]
    return turn, small, np.stack(parts)


def dft4(a, sign):
    (r0, i0), (r1, i1), (r2, i2), (r3, i3) = a
    s0r, s0i, d0r, d0i = r0 + r2, i0 + i2, r0 - r2, i0 - i2
    s1r, s1i, d1r, d1i = r1 + r3, i1 + i3, r1 - r3, i1 - i3
    up, down = (d0r - d1i, d0i + d1r), (d0r + d1i, d0i - d1r)
    first, third = (up, down) if sign > 0 else (down, up)
    return [(s0r + s1r, s0i + s1i), first, (s0r - s1r, s0i - s1i), third]


def dft32(re, im, small_ref, sign):
    half = math.sqrt(0.5)
    columns = dft4([(re[8 * n : 8 * n + 8], im[8 * n : 8 * n + 8]) for n in range(4)], sign)
    turned = [columns[0]]
    for k in range(1, 4):
        r, i = columns[k]
        c, s = small_ref[0, k - 1], small_ref[1, k - 1]
        turned.append((r * c + i * s, i * c - r * s) if sign < 0 else (r * c - i * s, i * c + r * s))
    re = jnp.stack([t[0] for t in turned])
    im = jnp.stack([t[1] for t in turned])
    rows = [(re[:, n], im[:, n]) for n in range(8)]
    even = dft4(rows[0::2], sign)
    odd = dft4(rows[1::2], sign)
    (r1, i1), (r2, i2), (r3, i3) = odd[1:]
    if sign < 0:
        odd = [odd[0], ((r1 + i1) * half, (i1 - r1) * half), (i2, -r2), ((i3 - r3) * half, (-r3 - i3) * half)]
    else:
        odd = [odd[0], ((r1 - i1) * half, (i1 + r1) * half), (-i2, r2), ((-r3 - i3) * half, (r3 - i3) * half)]
    result = [(e[0] + o[0], e[1] + o[1]) for e, o in zip(even, odd)]
    return result + [(e[0] - o[0], e[1] - o[1]) for e, o in zip(even, odd)]


def joined(pieces):
    return jnp.concatenate([p[0] for p in pieces]), jnp.concatenate([p[1] for p in pieces])


def split_dot(left, w_ref, which):
    top = left.astype(BF16)
    rest = (left - top.astype(F32)).astype(BF16)
    w_top, w_rest = w_ref[which], w_ref[which + 1]
    dot = functools.partial(jnp.dot, preferred_element_type=F32)
    return dot(top, w_top) + (dot(rest, w_top) + dot(top, w_rest))


def along_lanes(re, im, w_ref, which):
    left = jnp.concatenate([re.reshape(8 * LOW, HIGH), im.reshape(8 * LOW, HIGH)], axis=1)
    result = split_dot(left, w_ref, which)
    return result[:, :HIGH].reshape(LOW, 8, HIGH), result[:, HIGH:].reshape(LOW, 8, HIGH)


def kernel(
    x_ref, mask_ref, level_ref, turn_ref, small_ref, w_ref, out_ref,
    xbuf, tbuf, send, recv, prop, part, ring, own, pair, final, final_in, mask_in, level_at, level_out, level_in,
    turn, small, w,
    x_sem, in_sem, send_sem, recv_sem, ring_send, ring_recv, pair_send, pair_recv, final_send, final_recv,
    par_send, par_recv,
):
    depth = lax.axis_index("depth")
    row = lax.axis_index("rows")
    z, y_lo = depth // 2, lax.rem(depth, 2)
    core, y_hi, x = lax.rem(row, 2), lax.rem(row // 2, 4), row // 8
    other = depth + 1 - 2 * y_lo
    up, down = lax.rem(depth + 2, 2 * Z), lax.rem(depth + 2 * Z - 2, 2 * Z)

    def peer(i):
        h = lax.rem(i, 4)
        to_y = lax.rem(y_hi + lax.rem(h, 2) * 2 + h // 2, 4)
        to_core = lax.rem(core + lax.rem(i // 4, 2), 2)
        to_x = lax.rem(x + i // 8, 4)
        return (to_x * 4 + to_y) * 2 + to_core

    def load(g):
        rows = pl.ds(pl.multiple_of(g * 32, 32), 32)
        return pltpu.make_async_copy(x_ref.at[0, :, rows, :], xbuf.at[:, rows, :], x_sem.at[g])

    load_small = pltpu.make_async_copy(small_ref, small, in_sem.at[0])
    load_turn = pltpu.make_async_copy(turn_ref, turn, in_sem.at[1])
    load_w = pltpu.make_async_copy(w_ref, w, in_sem.at[2])
    load_level = pltpu.make_async_copy(level_ref, level_at, in_sem.at[3])
    load_small.start()
    load(0).start()
    load_turn.start()
    for g in range(1, 4):
        load(g).start()
    load_w.start()
    load_level.start()

    barrier = pltpu.get_barrier_semaphore()

    def greet(i, c):
        pl.semaphore_signal(barrier, inc=1, device_id=(other, i), device_id_type=MESH)
        return c

    lax.fori_loop(0, 32, greet, 0)
    pl.semaphore_signal(barrier, inc=1, device_id=(up, row), device_id_type=MESH)
    pl.semaphore_signal(barrier, inc=1, device_id=(down, row), device_id_type=MESH)

    load_small.wait()
    load_turn.wait()

    def width_first(t, c):
        rows = pl.ds(pl.multiple_of(t * 8, 8), 8)
        cells = [jnp.stack([xbuf[k, rows, a * HIGH : (a + 1) * HIGH] for a in range(LOW)]) for k in range(2)]
        re, im = joined(dft32(cells[0], cells[1], small, -1))
        cosine, sine = turn[0], turn[1]
        tbuf[:, 0, rows, :] = re * cosine + im * sine
        tbuf[:, 1, rows, :] = im * cosine - re * sine
        return c

    def width_group(g, c):
        load(g).wait()
        return lax.fori_loop(g * 4, g * 4 + 4, width_first, c)

    with jax.named_scope("A1"):
        lax.fori_loop(0, 4, width_group, 0)

    load_level.wait()
    level_out[...] = jnp.full((8, HIGH), level_at[0].astype(F32))
    load_w.wait()
    with jax.named_scope("barrier"):
        pl.semaphore_wait(barrier, 34)

    def exchange(q, t0, n, to):
        tiles = pl.ds(t0, n)
        return pltpu.make_async_remote_copy(
            send.at[tiles, to], recv.at[tiles, row], send_sem.at[q], recv_sem.at[q],
            device_id=(other, to), device_id_type=MESH,
        )

    def exchange_whole(q, t0, n):
        tiles = pl.ds(t0, n)
        return pltpu.make_async_remote_copy(
            send.at[tiles], recv.at[tiles], send_sem.at[q], recv_sem.at[q],
            device_id=(other, row), device_id_type=MESH,
        )

    def exchange_all(q, t0, n):
        def some(i, c):
            for h in range(4):
                exchange(q, t0, n, peer(i * 4 + h)).start()
            return c

        lax.fori_loop(0, 8, some, 0)

    def width_last(g, c):
        @pl.when(g > 0)
        def _():
            for h in range(4):
                exchange(0, 0, 2, peer((g - 1) * 4 + h)).start()

        for h in range(4):
            to = peer(g * 4 + h)
            both = split_dot(jnp.concatenate([tbuf[to, 0], tbuf[to, 1]], axis=1), w, 0)
            for k in range(2):
                send[:, to, k] = both[:, k * HIGH : (k + 1) * HIGH].T.reshape(TILES, 8, HIGH)
        return c

    with jax.named_scope("A2"):
        lax.fori_loop(0, 8, width_last, 0)
    mask_copy = pltpu.make_async_remote_copy(
        mask_ref, mask_in, par_send.at[0], par_recv.at[0], device_id=(other, row), device_id_type=MESH
    )
    level_copy = pltpu.make_async_remote_copy(
        level_out, level_in, par_send.at[1], par_recv.at[1], device_id=(other, row), device_id_type=MESH
    )
    mask_copy.start()
    level_copy.start()
    lax.fori_loop(28, 32, lambda i, c: (exchange(0, 0, 2, peer(i)).start(), c)[1], 0)
    exchange_all(1, 2, 2)

    mask_copy.wait()
    level_copy.wait()
    distance = 100.0 + 2.0 * level_in[...]

    def cutoff(k):
        total = jnp.sum(mask_in[0, k : k + 1, :].astype(F32), axis=1, keepdims=True)
        return jnp.broadcast_to((total + 1.0) * 0.5, (8, HIGH))[None]

    cut_y, cut_x = cutoff(0), cutoff(1)
    shape = (8, 8, HIGH)

    def signed(k):
        return jnp.where(k < N // 2, k, k - N).astype(F32)

    def propagate(i, c):
        t, g = i // 4, lax.rem(i, 4)
        k_y = signed(lax.broadcasted_iota(jnp.int32, shape, 0) + g * 8 + 32 * lax.broadcasted_iota(jnp.int32, shape, 2))
        k_x = signed(row + 32 * (t * 8 + lax.broadcasted_iota(jnp.int32, shape, 1)))
        f_y, f_x = k_y * (1.0 / N), k_x * (1.0 / N)
        square = f_y * f_y + f_x * f_x
        quarters = (-4.0 * distance[None]) * (square / (2.0 + jnp.sqrt(4.0 - square)))
        whole = jnp.floor(quarters + 0.5)
        v = (quarters - whole) * (0.5 * math.pi)
        quadrant = whole - 4.0 * jnp.floor(whole * 0.25)
        v2 = v * v
        sine = v + v * v2 * (-1.6666654611e-1 + v2 * (8.3321608736e-3 - v2 * 1.9515295891e-4))
        cosine = 1.0 - 0.5 * v2 + v2 * v2 * (4.166664568298827e-2 + v2 * (-1.388731625493765e-3 + v2 * 2.443315711809948e-5))
        odd = (quadrant == 1.0) | (quadrant == 3.0)
        re = jnp.where(odd, sine, cosine)
        im = jnp.where(odd, cosine, sine)
        inside = (jnp.abs(k_y) < cut_y) & (jnp.abs(k_x) < cut_x)
        weight = jnp.where(inside, 1.0, 0.0)
        prop[t, pl.ds(g * 8, 8), 0] = jnp.where((quadrant == 1.0) | (quadrant == 2.0), -re, re) * weight
        prop[t, pl.ds(g * 8, 8), 1] = jnp.where(quadrant >= 2.0, -im, im) * weight
        return c

    with jax.named_scope("H"):
        lax.fori_loop(0, 4 * TILES, propagate, 0)

    def height(t, c):
        re, im = joined(dft32(recv[t, :, 0], recv[t, :, 1], small, -1))
        cosine, sine = turn[0], turn[1]
        re, im = along_lanes(re * cosine + im * sine, im * cosine - re * sine, w, 0)
        p_re, p_im = prop[t, :, 0], prop[t, :, 1]
        re, im = along_lanes(re * p_re - im * p_im, re * p_im + im * p_re, w, 2)
        re, im = joined(dft32(re * cosine - im * sine, im * cosine + re * sine, small, 1))
        part[t, :, 0] = re
        part[t, :, 1] = im
        return c

    def ring_copy(q, t0, n, step, source):
        tiles = pl.ds(t0, n)
        return pltpu.make_async_remote_copy(
            part.at[tiles, pl.ds(source * 4, 4)], ring.at[tiles, step], ring_send.at[q, step], ring_recv.at[q, step],
            device_id=(up if step < 4 else down, row), device_id_type=MESH,
        )

    def ring_step(q, t0, n, step):
        tiles = pl.ds(t0, n)
        lines = [(step, lax.rem(z + 4 - step, Z))] + ([(step + 4, lax.rem(z + 5 + step, Z))] if step < 3 else [])
        for i, source in lines:
            if step > 0:
                ring_copy(q, t0, n, i - 1, source).wait_recv()
                block = pl.ds(source * 4, 4)
                part[tiles, block] = part[tiles, block] + ring[tiles, i - 1]
        for i, source in lines:
            ring_copy(q, t0, n, i, source).start()

    def pair_copy(q, t0, n):
        tiles = pl.ds(t0, n)
        return pltpu.make_async_remote_copy(
            own.at[tiles, pl.ds(y_lo * 2, 2)], pair.at[tiles], pair_send.at[q], pair_recv.at[q],
            device_id=(other, row), device_id_type=MESH,
        )

    def ring_end(q, t0, n):
        tiles = pl.ds(t0, n)
        ring_copy(q, t0, n, 6, z).wait_recv()
        ring_copy(q, t0, n, 3, z).wait_recv()
        own[tiles] = part[tiles, pl.ds(z * 4, 4)] + (ring[tiles, 3] + ring[tiles, 6])
        pair_copy(q, t0, n).start()

    def chunk(q, t0, n, before, ahead, between=None):
        with jax.named_scope("wait_a2a"):
            exchange_whole(q, t0, n).wait_recv()
        with jax.named_scope("C"):
            lax.fori_loop(t0, t0 + n, height, 0)
        ring_step(q, t0, n, 0)
        ahead()
        with jax.named_scope("ring"):
            if before is not None:
                ring_step(*before, 3)
            ring_step(q, t0, n, 1)
            if between is not None:
                between()
            if before is not None:
                ring_end(*before)
            ring_step(q, t0, n, 2)

    keep = 2 - 2 * y_lo

    def deliver(half, to):
        return pltpu.make_async_remote_copy(
            final.at[half, to], final_in.at[half, row], final_send.at[half], final_recv.at[half],
            device_id=(other, to), device_id_type=MESH,
        )

    def deliver_whole(half):
        return pltpu.make_async_remote_copy(
            final.at[half], final_in.at[half], final_send.at[half], final_recv.at[half],
            device_id=(other, row), device_id_type=MESH,
        )

    def hand_over(half):
        tiles = pl.ds(half * 8, 8)
        for a in range(2):
            block = [(own[tiles, keep + a, k] + pair[tiles, a, k]).reshape(64, HIGH) for k in range(2)]
            final[half, a * 16 : a * 16 + 16] = jnp.concatenate(block).T.reshape(16, 8, HIGH)

        def some(i, c):
            for h in range(4):
                deliver(half, peer(i * 4 + h)).start()
            return c

        lax.fori_loop(0, 8, some, 0)

    def first_half():
        for q in range(4):
            pair_copy(q, 2 * q, 2).wait_recv()
        hand_over(0)

    chunk(0, 0, 2, None, lambda: exchange_all(2, 4, 2))

    def middle(q, c):
        def ahead():
            @pl.when(q < WIDE - 2)
            def _():
                exchange_all(q + 2, 2 * q + 4, 2)

            @pl.when(q >= WIDE - 2)
            def _():
                exchange_all(q + 2, q + 2 + WIDE, 1)

        chunk(q, 2 * q, 2, (q - 1, 2 * q - 2, 2), ahead)
        return c

    lax.fori_loop(1, WIDE, middle, 0)
    chunk(WIDE, 14, 1, (WIDE - 1, 12, 2), lambda: None)
    chunk(WIDE + 1, 15, 1, (WIDE, 14, 1), lambda: None, first_half)
    with jax.named_scope("last_ring"):
        ring_step(WIDE + 1, 15, 1, 3)
        ring_end(WIDE + 1, 15, 1)
    with jax.named_scope("pair_wait"):
        for q in range(4, WIDE):
            pair_copy(q, 2 * q, 2).wait_recv()
        for q in range(WIDE, CHUNKS):
            pair_copy(q, q + WIDE, 1).wait_recv()
    hand_over(1)

    def settle(q, t0, n):
        exchange_whole(q, t0, n).wait_send()
        pair_copy(q, t0, n).wait_send()
        for step in range(7):
            ring_copy(q, t0, n, step, z).wait_send()

    lax.fori_loop(0, WIDE, lambda q, c: (settle(q, 2 * q, 2), c)[1], 0)
    for q in range(WIDE, CHUNKS):
        settle(q, q + WIDE, 1)
    with jax.named_scope("final_wait"):
        deliver_whole(0).wait_recv()
        deliver_whole(1).wait_recv()

    left = jnp.concatenate([final_in[0].reshape(8 * LOW, HIGH), final_in[1].reshape(8 * LOW, HIGH)], axis=1)
    both = split_dot(left, w, 4)
    re, im = both[:, :HIGH].reshape(LOW, 8, HIGH), both[:, HIGH:].reshape(LOW, 8, HIGH)
    cosine, sine = turn[0] * 0.25, turn[1] * 0.25
    pieces = dft32(re * cosine - im * sine, im * cosine + re * sine, small, 1)
    for k in range(8):
        for j in range(4):
            lanes = pl.ds((k * 4 + j) * HIGH, HIGH)
            out_ref[0, :, lanes] = pieces[k][0][j]
            out_ref[1, :, lanes] = pieces[k][1][j]
    deliver_whole(0).wait_send()
    deliver_whole(1).wait_send()


def local(target, depth_index, band_mask):
    turn, small, matrices = tables()
    anywhere = pl.BlockSpec(memory_space=pl.ANY)
    dma = pltpu.SemaphoreType.DMA
    return pl.pallas_call(
        kernel,
        out_shape=jax.ShapeDtypeStruct((2, 8, N), F32),
        in_specs=[anywhere] * 6,
        out_specs=pl.BlockSpec(memory_space=pltpu.VMEM),
        scratch_shapes=[
            pltpu.VMEM((2, HIGH, N), F32),
            pltpu.VMEM((LOW, 2, HIGH, HIGH), F32),
            pltpu.VMEM((TILES, LOW, 2, 8, HIGH), F32),
            pltpu.VMEM((TILES, LOW, 2, 8, HIGH), F32),
            pltpu.VMEM((TILES, LOW, 2, 8, HIGH), F32),
            pltpu.VMEM((TILES, LOW, 2, 8, HIGH), F32),
            pltpu.VMEM((TILES, 7, 4, 2, 8, HIGH), F32),
            pltpu.VMEM((TILES, 4, 2, 8, HIGH), F32),
            pltpu.VMEM((TILES, 2, 2, 8, HIGH), F32),
            pltpu.VMEM((2, LOW, 8, HIGH), F32),
            pltpu.VMEM((2, LOW, 8, HIGH), F32),
            pltpu.VMEM((1, 2, N), jnp.int32),
            pltpu.SMEM((1,), jnp.int32),
            pltpu.VMEM((8, HIGH), F32),
            pltpu.VMEM((8, HIGH), F32),
            pltpu.VMEM(turn.shape, F32),
            pltpu.VMEM(small.shape, F32),
            pltpu.VMEM(matrices.shape, BF16),
            dma((4,)),
            dma((4,)),
            dma((CHUNKS,)),
            dma((CHUNKS,)),
            dma((CHUNKS, 7)),
            dma((CHUNKS, 7)),
            dma((CHUNKS,)),
            dma((CHUNKS,)),
            dma((2,)),
            dma((2,)),
            dma((2,)),
            dma((2,)),
        ],
        compiler_params=pltpu.CompilerParams(
            collective_id=0, has_side_effects=True, vmem_limit_bytes=60 * 1024 * 1024
        ),
        name="hologram",
    )(target, band_mask, depth_index, turn, small, matrices)


def solution(mesh):
    in_specs = (P("depth", None, "rows", None), P("depth"), P("depth", None, None))
    out_specs = P(None, ("depth", "rows"), None)
    return jax.shard_map(local, mesh=mesh, in_specs=in_specs, out_specs=out_specs, check_vma=False)
```

```python
import functools
import math

import jax
import jax.numpy as jnp
import ml_dtypes
import numpy as np
from jax import lax
from jax.experimental import pallas as pl
from jax.experimental.pallas import tpu as pltpu
from jax.sharding import PartitionSpec as P

MESH = pl.DeviceIdType.MESH
N = 4096
LOW = 32
HIGH = 128
Z = 8
TILES = 16
WIDE = 7
CHUNKS = WIDE + 2
LAST = TILES - 1
FAR = (4, 3, 5, 2, 6, 1, 7)
F32 = jnp.float32
BF16 = jnp.bfloat16


def tables():
    angle = 2.0 * np.pi / N * np.outer(np.arange(LOW), np.arange(HIGH))
    turn = np.stack([np.cos(angle), np.sin(angle)]) / 64.0
    turn = np.broadcast_to(turn[:, :, None, :], (2, LOW, 8, HIGH)).astype(np.float32)
    angle = 2.0 * np.pi / LOW * np.outer(np.arange(1, 4), np.arange(8))
    small = np.stack([np.cos(angle), np.sin(angle)])
    small = np.broadcast_to(small[:, :, :, None, None], (2, 3, 8, 8, HIGH)).astype(np.float32)
    angle = 2.0 * np.pi / HIGH * (np.outer(np.arange(HIGH), np.arange(HIGH)) % HIGH)
    cosine, sine = np.cos(angle), np.sin(angle)
    ahead = np.block([[cosine, -sine], [sine, cosine]])
    parts = []
    for matrix in (ahead, ahead.T):
        top = matrix.astype(np.float32).astype(ml_dtypes.bfloat16)
        rest = (matrix - top.astype(np.float64)).astype(np.float32).astype(ml_dtypes.bfloat16)
        parts += [top, rest]
    order = np.arange(256).reshape(2, 2, 64).swapaxes(0, 1).reshape(256)
    parts += [parts[2][order], parts[3][order]]
    angle = 2.0 * np.pi / LOW * np.outer(np.arange(LOW), np.arange(LOW))
    cosine, sine = np.cos(angle), np.sin(angle)
    short = np.block([[cosine, -sine], [sine, cosine]])
    short = short.reshape(2, Z, 4, 2 * LOW).swapaxes(0, 1).reshape(2 * LOW, 2 * LOW)
    top = short.astype(np.float32).astype(ml_dtypes.bfloat16)
    rest = (short - top.astype(np.float64)).astype(np.float32).astype(ml_dtypes.bfloat16)
    return turn, small, np.stack(parts), turn[:, :, 0, :].copy(), np.stack([top, rest])


def dft4(a, sign):
    (r0, i0), (r1, i1), (r2, i2), (r3, i3) = a
    s0r, s0i, d0r, d0i = r0 + r2, i0 + i2, r0 - r2, i0 - i2
    s1r, s1i, d1r, d1i = r1 + r3, i1 + i3, r1 - r3, i1 - i3
    up, down = (d0r - d1i, d0i + d1r), (d0r + d1i, d0i - d1r)
    first, third = (up, down) if sign > 0 else (down, up)
    return [(s0r + s1r, s0i + s1i), first, (s0r - s1r, s0i - s1i), third]


def dft32(re, im, small_ref, sign):
    half = math.sqrt(0.5)
    columns = dft4([(re[8 * n : 8 * n + 8], im[8 * n : 8 * n + 8]) for n in range(4)], sign)
    turned = [columns[0]]
    for k in range(1, 4):
        r, i = columns[k]
        c, s = small_ref[0, k - 1], small_ref[1, k - 1]
        turned.append((r * c + i * s, i * c - r * s) if sign < 0 else (r * c - i * s, i * c + r * s))
    re = jnp.stack([t[0] for t in turned])
    im = jnp.stack([t[1] for t in turned])
    rows = [(re[:, n], im[:, n]) for n in range(8)]
    even = dft4(rows[0::2], sign)
    odd = dft4(rows[1::2], sign)
    (r1, i1), (r2, i2), (r3, i3) = odd[1:]
    if sign < 0:
        odd = [odd[0], ((r1 + i1) * half, (i1 - r1) * half), (i2, -r2), ((i3 - r3) * half, (-r3 - i3) * half)]
    else:
        odd = [odd[0], ((r1 - i1) * half, (i1 + r1) * half), (-i2, r2), ((-r3 - i3) * half, (r3 - i3) * half)]
    result = [(e[0] + o[0], e[1] + o[1]) for e, o in zip(even, odd)]
    return result + [(e[0] - o[0], e[1] - o[1]) for e, o in zip(even, odd)]


def joined(pieces):
    return jnp.concatenate([p[0] for p in pieces]), jnp.concatenate([p[1] for p in pieces])


def split_dot(left, w_ref, which):
    top = left.astype(BF16)
    rest = (left - top.astype(F32)).astype(BF16)
    w_top, w_rest = w_ref[which], w_ref[which + 1]
    dot = functools.partial(jnp.dot, preferred_element_type=F32)
    return dot(top, w_top) + (dot(rest, w_top) + dot(top, w_rest))


def along_lanes(re, im, w_ref, which):
    left = jnp.concatenate([re.reshape(8 * LOW, HIGH), im.reshape(8 * LOW, HIGH)], axis=1)
    result = split_dot(left, w_ref, which)
    return result[:, :HIGH].reshape(LOW, 8, HIGH), result[:, HIGH:].reshape(LOW, 8, HIGH)


def kernel(
    x_ref, mask_ref, level_ref, turn_ref, small_ref, w_ref, flat_ref, short_ref, out_ref,
    xbuf, tbuf, send, recv, prop, part, ring, own, pair, final, final_in, mask_in, level_at, level_out, level_in,
    turn, small, w, flat, short, z_out, z_in, par_out, par_in, sum_out, sum_in,
    x_sem, in_sem, send_sem, recv_sem, ring_send, ring_recv, pair_send, pair_recv, final_send, final_recv,
    par_send, par_recv, z_send, z_recv, all_send, all_recv, sum_send, sum_recv,
):
    depth = lax.axis_index("depth")
    row = lax.axis_index("rows")
    z, y_lo = depth // 2, lax.rem(depth, 2)
    core, y_hi, x = lax.rem(row, 2), lax.rem(row // 2, 4), row // 8
    other = depth + 1 - 2 * y_lo
    up, down = lax.rem(depth + 2, 2 * Z), lax.rem(depth + 2 * Z - 2, 2 * Z)

    def peer(i):
        h = lax.rem(i, 4)
        to_y = lax.rem(y_hi + lax.rem(h, 2) * 2 + h // 2, 4)
        to_core = lax.rem(core + lax.rem(i // 4, 2), 2)
        to_x = lax.rem(x + i // 8, 4)
        return (to_x * 4 + to_y) * 2 + to_core

    xs = [lax.rem(x + k, 4) for k in range(4)]
    ys = [lax.rem(y_hi + y_lo + k, 4) for k in range(4)]
    cores = [core, 1 - core]
    near_first = [(xs[i] * 4 + ys[h]) * 2 + c for i in range(4) for c in cores for h in (1, 2, 0, 3)]
    far_first = [(xs[i] * 4 + ys[h]) * 2 + c for i in (2, 1, 3, 0) for h in (1, 2, 0, 3) for c in cores]

    def load(g):
        rows = pl.ds(pl.multiple_of(g * 32, 32), 32)
        return pltpu.make_async_copy(x_ref.at[0, :, rows, :], xbuf.at[:, rows, :], x_sem.at[g])

    load_small = pltpu.make_async_copy(small_ref, small, in_sem.at[0])
    load_turn = pltpu.make_async_copy(turn_ref, turn, in_sem.at[1])
    load_w = pltpu.make_async_copy(w_ref, w, in_sem.at[2])
    load_level = pltpu.make_async_copy(level_ref, level_at, in_sem.at[3])
    load_small.start()
    load(0).start()
    load_turn.start()
    for g in range(1, 4):
        load(g).start()
    load_w.start()
    load_level.start()
    load_flat = pltpu.make_async_copy(flat_ref, flat, in_sem.at[4])
    load_short = pltpu.make_async_copy(short_ref, short, in_sem.at[5])
    load_flat.start()
    load_short.start()

    barrier = pltpu.get_barrier_semaphore()

    def greet(i, c):
        pl.semaphore_signal(barrier, inc=1, device_id=(other, i), device_id_type=MESH)
        return c

    lax.fori_loop(0, 32, greet, 0)
    for k in FAR:
        pl.semaphore_signal(barrier, inc=1, device_id=(2 * lax.rem(z + k, Z) + y_lo, row), device_id_type=MESH)

    load_small.wait()
    load_turn.wait()

    def width_first(t, c):
        rows = pl.ds(pl.multiple_of(t * 8, 8), 8)
        cells = [jnp.stack([xbuf[k, rows, a * HIGH : (a + 1) * HIGH] for a in range(LOW)]) for k in range(2)]
        re, im = joined(dft32(cells[0], cells[1], small, -1))
        cosine, sine = turn[0], turn[1]
        tbuf[:, 0, rows, :] = re * cosine + im * sine
        tbuf[:, 1, rows, :] = im * cosine - re * sine
        return c

    def width_group(g, c):
        load(g).wait()
        return lax.fori_loop(g * 4, g * 4 + 4, width_first, c)

    with jax.named_scope("A1"):
        lax.fori_loop(0, 4, width_group, 0)

    load_level.wait()
    level_out[...] = jnp.full((8, HIGH), level_at[0].astype(F32))
    load_w.wait()
    load_flat.wait()
    load_short.wait()
    with jax.named_scope("barrier"):
        pl.semaphore_wait(barrier, 39)

    def exchange(q, t0, n, to):
        tiles = pl.ds(t0, n)
        return pltpu.make_async_remote_copy(
            send.at[tiles, to], recv.at[tiles, row], send_sem.at[q], recv_sem.at[q],
            device_id=(other, to), device_id_type=MESH,
        )

    def exchange_whole(q, t0, n):
        tiles = pl.ds(t0, n)
        return pltpu.make_async_remote_copy(
            send.at[tiles], recv.at[tiles], send_sem.at[q], recv_sem.at[q],
            device_id=(other, row), device_id_type=MESH,
        )

    def exchange_all(q, t0, n):
        for to in near_first:
            exchange(q, t0, n, to).start()

    def along_z(out, into, send_sems, recv_sems, k, shared=False):
        to = lax.rem(z + k, Z)
        return pltpu.make_async_remote_copy(
            out if shared else out.at[to], into.at[z], send_sems.at[k], recv_sems.at[z],
            device_id=(2 * to + y_lo, row), device_id_type=MESH,
        )

    def from_z(out, into, send_sems, recv_sems, k, shared=False):
        source = lax.rem(z + k, Z)
        return pltpu.make_async_remote_copy(
            out if shared else out.at[source], into.at[source], send_sems.at[k], recv_sems.at[source],
            device_id=(2 * source + y_lo, row), device_id_type=MESH,
        )

    def width_last(g, c):
        @pl.when(g > 0)
        def _():
            for h in range(4):
                exchange(0, 0, 2, peer((g - 1) * 4 + h)).start()

        for h in range(4):
            to = peer(g * 4 + h)
            both = split_dot(jnp.concatenate([tbuf[to, 0], tbuf[to, 1]], axis=1), w, 0)
            for k in range(2):
                send[:, to, k] = both[:, k * HIGH : (k + 1) * HIGH].T.reshape(TILES, 8, HIGH)
        return c

    with jax.named_scope("A2"):
        lax.fori_loop(0, 8, width_last, 0)
    for g in range(8):
        block = send[LAST, 4 * g : 4 * g + 4].reshape(8, 8, HIGH)
        z_out[:, 8 * g : 8 * g + 8, :] = jnp.swapaxes(block, 0, 1)
    mask_copy = pltpu.make_async_remote_copy(
        mask_ref, mask_in, par_send.at[0], par_recv.at[0], device_id=(other, row), device_id_type=MESH
    )
    level_copy = pltpu.make_async_remote_copy(
        level_out, level_in, par_send.at[1], par_recv.at[1], device_id=(other, row), device_id_type=MESH
    )
    mask_copy.start()
    level_copy.start()
    lax.fori_loop(28, 32, lambda i, c: (exchange(0, 0, 2, peer(i)).start(), c)[1], 0)
    for k in FAR:
        along_z(z_out, z_in, z_send, z_recv, k).start()
    z_in[z] = z_out[z]
    exchange_all(1, 2, 2)

    mask_copy.wait()
    level_copy.wait()
    distance = 100.0 + 2.0 * level_in[...]

    def cutoff(k):
        total = jnp.sum(mask_in[0, k : k + 1, :].astype(F32), axis=1, keepdims=True)
        return jnp.broadcast_to((total + 1.0) * 0.5, (8, HIGH))

    cut_y, cut_x = cutoff(0), cutoff(1)
    line = lax.broadcasted_iota(jnp.int32, (8, HIGH), 0)
    about = jnp.where(line == 0, distance, jnp.where(line == 1, cut_y, cut_x))
    par_out[...] = about
    par_in[z] = about
    shape = (8, 8, HIGH)

    def signed(k):
        return jnp.where(k < N // 2, k, k - N).astype(F32)

    def propagate(t, g, k_x, distance, cut_y, cut_x):
        k_y = signed(lax.broadcasted_iota(jnp.int32, shape, 0) + g * 8 + 32 * lax.broadcasted_iota(jnp.int32, shape, 2))
        f_y, f_x = k_y * (1.0 / N), k_x * (1.0 / N)
        square = f_y * f_y + f_x * f_x
        quarters = (-4.0 * distance[None]) * (square / (2.0 + jnp.sqrt(4.0 - square)))
        whole = jnp.floor(quarters + 0.5)
        v = (quarters - whole) * (0.5 * math.pi)
        quadrant = whole - 4.0 * jnp.floor(whole * 0.25)
        v2 = v * v
        sine = v + v * v2 * (-1.6666654611e-1 + v2 * (8.3321608736e-3 - v2 * 1.9515295891e-4))
        cosine = 1.0 - 0.5 * v2 + v2 * v2 * (4.166664568298827e-2 + v2 * (-1.388731625493765e-3 + v2 * 2.443315711809948e-5))
        odd = (quadrant == 1.0) | (quadrant == 3.0)
        re = jnp.where(odd, sine, cosine)
        im = jnp.where(odd, cosine, sine)
        inside = (jnp.abs(k_y) < cut_y[None]) & (jnp.abs(k_x) < cut_x[None])
        weight = jnp.where(inside, 1.0, 0.0)
        prop[t, pl.ds(g * 8, 8), 0] = jnp.where((quadrant == 1.0) | (quadrant == 2.0), -re, re) * weight
        prop[t, pl.ds(g * 8, 8), 1] = jnp.where(quadrant >= 2.0, -im, im) * weight

    def propagate_tile(i, c):
        t, g = i // 4, lax.rem(i, 4)
        k_x = signed(row + 32 * (t * 8 + lax.broadcasted_iota(jnp.int32, shape, 1)))
        propagate(t, g, k_x, distance, cut_y, cut_x)
        return c

    with jax.named_scope("H"):
        lax.fori_loop(0, 4 * LAST, propagate_tile, 0)
    for k in FAR:
        along_z(par_out, par_in, all_send, all_recv, k, True).start()

    def prepare_last():
        for k in FAR:
            from_z(z_out, z_in, z_send, z_recv, k).wait_recv()
            from_z(par_out, par_in, all_send, all_recv, k, True).wait_recv()
        for g in range(8):
            send[LAST, 4 * g : 4 * g + 4] = jnp.swapaxes(z_in[:, 8 * g : 8 * g + 8, :], 0, 1).reshape(4, 2, 8, HIGH)
        each = [jnp.concatenate([par_in[p, j : j + 1, :] for p in range(8)]) for j in range(3)]
        k_x = signed(jnp.full(shape, row + 32 * (8 * LAST + z), jnp.int32))

        def group(g, c):
            propagate(LAST, g, k_x, *each)
            return c

        lax.fori_loop(0, 4, group, 0)

    def height(t, c):
        re, im = joined(dft32(recv[t, :, 0], recv[t, :, 1], small, -1))
        cosine, sine = turn[0], turn[1]
        re, im = along_lanes(re * cosine + im * sine, im * cosine - re * sine, w, 0)
        p_re, p_im = prop[t, :, 0], prop[t, :, 1]
        re, im = along_lanes(re * p_re - im * p_im, re * p_im + im * p_re, w, 2)
        re, im = joined(dft32(re * cosine - im * sine, im * cosine + re * sine, small, 1))
        part[t, :, 0] = re
        part[t, :, 1] = im
        return c

    def height_last():
        re, im = joined(dft32(recv[LAST, :, 0], recv[LAST, :, 1], small, -1))
        cosine, sine = turn[0], turn[1]
        re, im = along_lanes(re * cosine + im * sine, im * cosine - re * sine, w, 0)
        p_re, p_im = prop[LAST, :, 0], prop[LAST, :, 1]
        left = jnp.concatenate(
            [jnp.sum(re * p_re - im * p_im, axis=1), jnp.sum(re * p_im + im * p_re, axis=1)], axis=1
        )
        both = split_dot(left, w, 2)
        re, im = both[:, :HIGH], both[:, HIGH:]
        cosine, sine = flat[0], flat[1]
        right = jnp.concatenate([re * cosine - im * sine, im * cosine + re * sine])
        top = right.astype(BF16)
        rest = (right - top.astype(F32)).astype(BF16)
        dot = functools.partial(jnp.dot, preferred_element_type=F32)
        result = dot(short[0], top) + (dot(short[0], rest) + dot(short[1], top))
        sum_out[...] = result.reshape(Z, 8, HIGH)
        sum_in[z] = sum_out[z]

    def ring_copy(q, t0, n, step, source):
        tiles = pl.ds(t0, n)
        return pltpu.make_async_remote_copy(
            part.at[tiles, pl.ds(source * 4, 4)], ring.at[tiles, step], ring_send.at[q, step], ring_recv.at[q, step],
            device_id=(up if step < 4 else down, row), device_id_type=MESH,
        )

    def ring_step(q, t0, n, step):
        tiles = pl.ds(t0, n)
        lines = [(step, lax.rem(z + 4 - step, Z))] + ([(step + 4, lax.rem(z + 5 + step, Z))] if step < 3 else [])
        for i, source in lines:
            if step > 0:
                ring_copy(q, t0, n, i - 1, source).wait_recv()
                block = pl.ds(source * 4, 4)
                part[tiles, block] = part[tiles, block] + ring[tiles, i - 1]
        for i, source in lines:
            ring_copy(q, t0, n, i, source).start()

    def pair_copy(q, t0, n):
        tiles = pl.ds(t0, n)
        return pltpu.make_async_remote_copy(
            own.at[tiles, pl.ds(y_lo * 2, 2)], pair.at[tiles], pair_send.at[q], pair_recv.at[q],
            device_id=(other, row), device_id_type=MESH,
        )

    def ring_end(q, t0, n):
        tiles = pl.ds(t0, n)
        ring_copy(q, t0, n, 6, z).wait_recv()
        ring_copy(q, t0, n, 3, z).wait_recv()
        own[tiles] = part[tiles, pl.ds(z * 4, 4)] + (ring[tiles, 3] + ring[tiles, 6])
        pair_copy(q, t0, n).start()

    def chunk(q, t0, n, before, ahead):
        with jax.named_scope("wait_a2a"):
            exchange_whole(q, t0, n).wait_recv()
        with jax.named_scope("C"):
            lax.fori_loop(t0, t0 + n, height, 0)
        ring_step(q, t0, n, 0)
        ahead()
        with jax.named_scope("ring"):
            if before is not None:
                ring_step(*before, 3)
            ring_step(q, t0, n, 1)
            if before is not None:
                ring_end(*before)
            if q is not WIDE:
                ring_step(q, t0, n, 2)

    keep = 2 - 2 * y_lo

    def deliver(half, to):
        return pltpu.make_async_remote_copy(
            final.at[half, to], final_in.at[half, row], final_send.at[half], final_recv.at[half],
            device_id=(other, to), device_id_type=MESH,
        )

    def deliver_whole(half):
        return pltpu.make_async_remote_copy(
            final.at[half], final_in.at[half], final_send.at[half], final_recv.at[half],
            device_id=(other, row), device_id_type=MESH,
        )

    def hand_over(half):
        tiles = pl.ds(half * 8, 8)
        for a in range(2):
            block = [(own[tiles, keep + a, k] + pair[tiles, a, k]).reshape(64, HIGH) for k in range(2)]
            final[half, a * 16 : a * 16 + 16] = jnp.concatenate(block).T.reshape(16, 8, HIGH)

    def dispatch(half):
        for to in far_first:
            deliver(half, to).start()

    chunk(0, 0, 2, None, lambda: exchange_all(2, 4, 2))

    def middle(q, c):
        def ahead():
            @pl.when(q == 3)
            def _():
                prepare_last()

            @pl.when(q < WIDE - 2)
            def _():
                exchange_all(q + 2, 2 * q + 4, 2)

            @pl.when(q >= WIDE - 2)
            def _():
                exchange_all(q + 2, q + 2 + WIDE, 1)

        chunk(q, 2 * q, 2, (q - 1, 2 * q - 2, 2), ahead)
        return c

    lax.fori_loop(1, WIDE, middle, 0)
    chunk(WIDE, 14, 1, (WIDE - 1, 12, 2), lambda: None)
    with jax.named_scope("first_half"):
        for q in range(4):
            pair_copy(q, 2 * q, 2).wait_recv()
        hand_over(0)
    with jax.named_scope("wait_last"):
        exchange_whole(WIDE + 1, LAST, 1).wait_recv()
    with jax.named_scope("C_last"):
        height_last()
    for k in FAR:
        along_z(sum_out, sum_in, sum_send, sum_recv, k).start()
    with jax.named_scope("last_ring"):
        ring_step(WIDE, 14, 1, 2)
        dispatch(0)
        ring_step(WIDE, 14, 1, 3)
    with jax.named_scope("last_sum"):
        for k in FAR:
            from_z(sum_out, sum_in, sum_send, sum_recv, k).wait_recv()
        lines = jnp.swapaxes(sum_in[...], 0, 1)
        for k in range(2):
            own[LAST, :, k] = lines[4 * k : 4 * k + 4]
        pair_copy(WIDE + 1, LAST, 1).start()
        ring_end(WIDE, 14, 1)
    with jax.named_scope("pair_wait"):
        for q in range(4, WIDE):
            pair_copy(q, 2 * q, 2).wait_recv()
        for q in range(WIDE, CHUNKS):
            pair_copy(q, q + WIDE, 1).wait_recv()
    hand_over(1)
    dispatch(1)

    def settle(q, t0, n):
        exchange_whole(q, t0, n).wait_send()
        pair_copy(q, t0, n).wait_send()
        if t0 is not LAST:
            for step in range(7):
                ring_copy(q, t0, n, step, z).wait_send()

    lax.fori_loop(0, WIDE, lambda q, c: (settle(q, 2 * q, 2), c)[1], 0)
    settle(WIDE, LAST - 1, 1)
    settle(WIDE + 1, LAST, 1)
    for k in FAR:
        along_z(z_out, z_in, z_send, z_recv, k).wait_send()
        along_z(par_out, par_in, all_send, all_recv, k, True).wait_send()
        along_z(sum_out, sum_in, sum_send, sum_recv, k).wait_send()
    with jax.named_scope("final_wait"):
        deliver_whole(0).wait_recv()
        deliver_whole(1).wait_recv()

    left = jnp.concatenate([final_in[0].reshape(8 * LOW, HIGH), final_in[1].reshape(8 * LOW, HIGH)], axis=1)
    both = split_dot(left, w, 4)
    re, im = both[:, :HIGH].reshape(LOW, 8, HIGH), both[:, HIGH:].reshape(LOW, 8, HIGH)
    cosine, sine = turn[0] * 0.25, turn[1] * 0.25
    pieces = dft32(re * cosine - im * sine, im * cosine + re * sine, small, 1)
    for k in range(8):
        for j in range(4):
            lanes = pl.ds((k * 4 + j) * HIGH, HIGH)
            out_ref[0, :, lanes] = pieces[k][0][j]
            out_ref[1, :, lanes] = pieces[k][1][j]
    deliver_whole(0).wait_send()
    deliver_whole(1).wait_send()


def local(target, depth_index, band_mask):
    turn, small, matrices, flat, short = tables()
    anywhere = pl.BlockSpec(memory_space=pl.ANY)
    dma = pltpu.SemaphoreType.DMA
    return pl.pallas_call(
        kernel,
        out_shape=jax.ShapeDtypeStruct((2, 8, N), F32),
        in_specs=[anywhere] * 8,
        out_specs=pl.BlockSpec(memory_space=pltpu.VMEM),
        scratch_shapes=[
            pltpu.VMEM((2, HIGH, N), F32),
            pltpu.VMEM((LOW, 2, HIGH, HIGH), F32),
            pltpu.VMEM((TILES, LOW, 2, 8, HIGH), F32),
            pltpu.VMEM((TILES, LOW, 2, 8, HIGH), F32),
            pltpu.VMEM((TILES, LOW, 2, 8, HIGH), F32),
            pltpu.VMEM((TILES, LOW, 2, 8, HIGH), F32),
            pltpu.VMEM((TILES, 7, 4, 2, 8, HIGH), F32),
            pltpu.VMEM((TILES, 4, 2, 8, HIGH), F32),
            pltpu.VMEM((TILES, 2, 2, 8, HIGH), F32),
            pltpu.VMEM((2, LOW, 8, HIGH), F32),
            pltpu.VMEM((2, LOW, 8, HIGH), F32),
            pltpu.VMEM((1, 2, N), jnp.int32),
            pltpu.SMEM((1,), jnp.int32),
            pltpu.VMEM((8, HIGH), F32),
            pltpu.VMEM((8, HIGH), F32),
            pltpu.VMEM(turn.shape, F32),
            pltpu.VMEM(small.shape, F32),
            pltpu.VMEM(matrices.shape, BF16),
            pltpu.VMEM(flat.shape, F32),
            pltpu.VMEM(short.shape, BF16),
            pltpu.VMEM((Z, 2 * LOW, HIGH), F32),
            pltpu.VMEM((Z, 2 * LOW, HIGH), F32),
            pltpu.VMEM((8, HIGH), F32),
            pltpu.VMEM((Z, 8, HIGH), F32),
            pltpu.VMEM((Z, 8, HIGH), F32),
            pltpu.VMEM((Z, 8, HIGH), F32),
            dma((4,)),
            dma((6,)),
            dma((CHUNKS,)),
            dma((CHUNKS,)),
            dma((CHUNKS, 7)),
            dma((CHUNKS, 7)),
            dma((CHUNKS,)),
            dma((CHUNKS,)),
            dma((2,)),
            dma((2,)),
            dma((2,)),
            dma((2,)),
            dma((Z,)),
            dma((Z,)),
            dma((Z,)),
            dma((Z,)),
            dma((Z,)),
            dma((Z,)),
        ],
        compiler_params=pltpu.CompilerParams(
            collective_id=0, has_side_effects=True, vmem_limit_bytes=60 * 1024 * 1024
        ),
        name="hologram",
    )(target, band_mask, depth_index, turn, small, matrices, flat, short)


def solution(mesh):
    in_specs = (P("depth", None, "rows", None), P("depth"), P("depth", None, None))
    out_specs = P(None, ("depth", "rows"), None)
    return jax.shard_map(local, mesh=mesh, in_specs=in_specs, out_specs=out_specs, check_vma=False)
```

```python
import functools
import math

import jax
import jax.numpy as jnp
import ml_dtypes
import numpy as np
from jax import lax
from jax.experimental import pallas as pl
from jax.experimental.pallas import tpu as pltpu
from jax.sharding import PartitionSpec as P

MESH = pl.DeviceIdType.MESH
N = 4096
LOW = 32
HIGH = 128
Z = 8
TILES = 16
WIDE = 6
SINGLE = 4
CHUNKS = WIDE + SINGLE
ALONE = 2 * WIDE
PAIRED = (0, 8, 15, 16)
FAR = (4, 3, 5, 2, 6, 1, 7)
F32 = jnp.float32
BF16 = jnp.bfloat16


def tables():
    angle = 2.0 * np.pi / N * np.outer(np.arange(LOW), np.arange(HIGH))
    turn = np.stack([np.cos(angle), np.sin(angle)]) / 64.0
    turn = np.broadcast_to(turn[:, :, None, :], (2, LOW, 8, HIGH)).astype(np.float32)
    angle = 2.0 * np.pi / LOW * np.outer(np.arange(1, 4), np.arange(8))
    small = np.stack([np.cos(angle), np.sin(angle)])
    small = np.broadcast_to(small[:, :, :, None, None], (2, 3, 8, 8, HIGH)).astype(np.float32)
    angle = 2.0 * np.pi / HIGH * (np.outer(np.arange(HIGH), np.arange(HIGH)) % HIGH)
    cosine, sine = np.cos(angle), np.sin(angle)
    ahead = np.block([[cosine, -sine], [sine, cosine]])
    parts = []
    for matrix in (ahead, ahead.T):
        top = matrix.astype(np.float32).astype(ml_dtypes.bfloat16)
        rest = (matrix - top.astype(np.float64)).astype(np.float32).astype(ml_dtypes.bfloat16)
        parts += [top, rest]
    order = np.arange(256).reshape(2, 2, 64).swapaxes(0, 1).reshape(256)
    parts += [parts[2][order], parts[3][order]]
    angle = 2.0 * np.pi / LOW * np.outer(np.arange(LOW), np.arange(LOW))
    cosine, sine = np.cos(angle), np.sin(angle)
    short = np.block([[cosine, -sine], [sine, cosine]])
    short = short.reshape(2, Z, 4, 2 * LOW).swapaxes(0, 1).reshape(2 * LOW, 2 * LOW)
    top = short.astype(np.float32).astype(ml_dtypes.bfloat16)
    rest = (short - top.astype(np.float64)).astype(np.float32).astype(ml_dtypes.bfloat16)
    return turn, small, np.stack(parts), turn[:, :, 0, :].copy(), np.stack([top, rest])


def dft4(a, sign):
    (r0, i0), (r1, i1), (r2, i2), (r3, i3) = a
    s0r, s0i, d0r, d0i = r0 + r2, i0 + i2, r0 - r2, i0 - i2
    s1r, s1i, d1r, d1i = r1 + r3, i1 + i3, r1 - r3, i1 - i3
    up, down = (d0r - d1i, d0i + d1r), (d0r + d1i, d0i - d1r)
    first, third = (up, down) if sign > 0 else (down, up)
    return [(s0r + s1r, s0i + s1i), first, (s0r - s1r, s0i - s1i), third]


def dft32(re, im, small_ref, sign):
    half = math.sqrt(0.5)
    columns = dft4([(re[8 * n : 8 * n + 8], im[8 * n : 8 * n + 8]) for n in range(4)], sign)
    turned = [columns[0]]
    for k in range(1, 4):
        r, i = columns[k]
        c, s = small_ref[0, k - 1], small_ref[1, k - 1]
        turned.append((r * c + i * s, i * c - r * s) if sign < 0 else (r * c - i * s, i * c + r * s))
    re = jnp.stack([t[0] for t in turned])
    im = jnp.stack([t[1] for t in turned])
    rows = [(re[:, n], im[:, n]) for n in range(8)]
    even = dft4(rows[0::2], sign)
    odd = dft4(rows[1::2], sign)
    (r1, i1), (r2, i2), (r3, i3) = odd[1:]
    if sign < 0:
        odd = [odd[0], ((r1 + i1) * half, (i1 - r1) * half), (i2, -r2), ((i3 - r3) * half, (-r3 - i3) * half)]
    else:
        odd = [odd[0], ((r1 - i1) * half, (i1 + r1) * half), (-i2, r2), ((-r3 - i3) * half, (r3 - i3) * half)]
    result = [(e[0] + o[0], e[1] + o[1]) for e, o in zip(even, odd)]
    return result + [(e[0] - o[0], e[1] - o[1]) for e, o in zip(even, odd)]


def joined(pieces):
    return jnp.concatenate([p[0] for p in pieces]), jnp.concatenate([p[1] for p in pieces])


def split_dot(left, w_ref, which, rows=slice(None)):
    top = left.astype(BF16)
    rest = (left - top.astype(F32)).astype(BF16)
    w_top, w_rest = w_ref[which, rows], w_ref[which + 1, rows]
    dot = functools.partial(jnp.dot, preferred_element_type=F32)
    return dot(top, w_top) + (dot(rest, w_top) + dot(top, w_rest))


def along_lanes(re, im, w_ref, which):
    left = jnp.concatenate([re.reshape(8 * LOW, HIGH), im.reshape(8 * LOW, HIGH)], axis=1)
    result = split_dot(left, w_ref, which)
    return result[:, :HIGH].reshape(LOW, 8, HIGH), result[:, HIGH:].reshape(LOW, 8, HIGH)


def kernel(
    x_ref, mask_ref, level_ref, turn_ref, small_ref, w_ref, flat_ref, short_ref, out_ref,
    xbuf, tbuf, send, recv, prop, part, ring, own, pair, final, final_in, mask_in, level_at, level_out, level_in,
    turn, small, w, flat, short, z_out, z_in, par_out, par_in, sum_out, sum_in,
    x_sem, in_sem, send_sem, recv_sem, ring_send, ring_recv, pair_send, pair_recv, final_send, final_recv,
    par_send, par_recv, z_send, z_recv, all_send, all_recv, sum_send, sum_recv,
):
    depth = lax.axis_index("depth")
    row = lax.axis_index("rows")
    z, y_lo = depth // 2, lax.rem(depth, 2)
    core, y_hi, x = lax.rem(row, 2), lax.rem(row // 2, 4), row // 8
    other = depth + 1 - 2 * y_lo
    up, down = lax.rem(depth + 2, 2 * Z), lax.rem(depth + 2 * Z - 2, 2 * Z)

    column = (x * 4 + lax.rem(y_hi + y_lo * core, 4)) * 2 + core
    mate = (x * 4 + lax.rem(y_hi + core * (3 - 2 * y_lo), 4)) * 2 + core

    def place(to_x, to_y, to_core):
        return (to_x * 4 + to_y) * 2 + to_core, (to_x * 4 + lax.rem(to_y + to_core * (1 - y_lo), 4)) * 2 + to_core

    def peer(i):
        h = lax.rem(i, 4)
        to_y = lax.rem(y_hi + lax.rem(h, 2) * 2 + h // 2, 4)
        to_core = lax.rem(core + lax.rem(i // 4, 2), 2)
        to_x = lax.rem(x + i // 8, 4)
        return place(to_x, to_y, to_core)

    xs = [lax.rem(x + k, 4) for k in range(4)]
    ys = [lax.rem(y_hi + y_lo + k, 4) for k in range(4)]
    cores = [core, 1 - core]
    near_first = [place(xs[i], ys[h], c) for i in range(4) for c in cores for h in (1, 2, 0, 3)]
    far_first = [place(xs[i], ys[h], c) for i in (2, 1, 3, 0) for h in (1, 2, 0, 3) for c in cores]

    def load(g):
        rows = pl.ds(pl.multiple_of(g * 32, 32), 32)
        return pltpu.make_async_copy(x_ref.at[0, :, rows, :], xbuf.at[:, rows, :], x_sem.at[g])

    load_small = pltpu.make_async_copy(small_ref, small, in_sem.at[0])
    load_turn = pltpu.make_async_copy(turn_ref, turn, in_sem.at[1])
    load_w = pltpu.make_async_copy(w_ref, w, in_sem.at[2])
    load_level = pltpu.make_async_copy(level_ref, level_at, in_sem.at[3])
    load_small.start()
    load(0).start()
    load_turn.start()
    for g in range(1, 4):
        load(g).start()
    load_w.start()
    load_level.start()
    load_flat = pltpu.make_async_copy(flat_ref, flat, in_sem.at[4])
    load_short = pltpu.make_async_copy(short_ref, short, in_sem.at[5])
    load_flat.start()
    load_short.start()

    barrier = pltpu.get_barrier_semaphore()

    def greet(i, c):
        pl.semaphore_signal(barrier, inc=1, device_id=(other, i), device_id_type=MESH)
        return c

    lax.fori_loop(0, 32, greet, 0)
    for k in FAR:
        pl.semaphore_signal(barrier, inc=1, device_id=(2 * lax.rem(z + k, Z) + y_lo, row), device_id_type=MESH)

    load_small.wait()
    load_turn.wait()

    def width_first(t, c):
        rows = pl.ds(pl.multiple_of(t * 8, 8), 8)
        cells = [jnp.stack([xbuf[k, rows, a * HIGH : (a + 1) * HIGH] for a in range(LOW)]) for k in range(2)]
        re, im = joined(dft32(cells[0], cells[1], small, -1))
        cosine, sine = turn[0], turn[1]
        tbuf[:, 0, rows, :] = re * cosine + im * sine
        tbuf[:, 1, rows, :] = im * cosine - re * sine
        return c

    def width_group(g, c):
        load(g).wait()
        return lax.fori_loop(g * 4, g * 4 + 4, width_first, c)

    with jax.named_scope("A1"):
        lax.fori_loop(0, 4, width_group, 0)

    load_level.wait()
    level_out[...] = jnp.full((8, HIGH), level_at[0].astype(F32))
    load_w.wait()
    load_flat.wait()
    load_short.wait()
    with jax.named_scope("barrier"):
        pl.semaphore_wait(barrier, 39)
    mask_copy = pltpu.make_async_remote_copy(
        mask_ref, mask_in, par_send.at[0], par_recv.at[0], device_id=(other, row), device_id_type=MESH
    )
    level_copy = pltpu.make_async_remote_copy(
        level_out, level_in, par_send.at[1], par_recv.at[1], device_id=(other, row), device_id_type=MESH
    )
    mask_copy.start()
    level_copy.start()

    def exchange(q, t0, n, to, block):
        tiles = pl.ds(t0, n)
        return pltpu.make_async_remote_copy(
            send.at[tiles, block], recv.at[tiles, row], send_sem.at[q], recv_sem.at[q],
            device_id=(other, to), device_id_type=MESH,
        )

    def exchange_whole(q, t0, n):
        tiles = pl.ds(t0, n)
        return pltpu.make_async_remote_copy(
            send.at[tiles], recv.at[tiles], send_sem.at[q], recv_sem.at[q],
            device_id=(other, row), device_id_type=MESH,
        )

    def exchange_all(q, t0, n):
        for to, block in near_first:
            exchange(q, t0, n, to, block).start()

    def along_z(out, into, send_sems, recv_sems, k, shared=False):
        to = lax.rem(z + k, Z)
        return pltpu.make_async_remote_copy(
            out if shared else out.at[to], into.at[z], send_sems.at[k], recv_sems.at[z],
            device_id=(2 * to + y_lo, row), device_id_type=MESH,
        )

    def from_z(out, into, send_sems, recv_sems, k, shared=False):
        source = lax.rem(z + k, Z)
        return pltpu.make_async_remote_copy(
            out if shared else out.at[source], into.at[source], send_sems.at[k], recv_sems.at[source],
            device_id=(2 * source + y_lo, row), device_id_type=MESH,
        )

    def width_last(g, c):
        @pl.when(g > 0)
        def _():
            for h in range(4):
                exchange(0, 0, 2, *peer((g - 1) * 4 + h)).start()

        for h in range(4):
            _, block = peer(g * 4 + h)
            both = split_dot(jnp.concatenate([tbuf[block, 0], tbuf[block, 1]], axis=1), w, 0)
            for k in range(2):
                send[:, block, k] = both[:, k * HIGH : (k + 1) * HIGH].T.reshape(TILES, 8, HIGH)
        return c

    with jax.named_scope("A2"):
        lax.fori_loop(0, 8, width_last, 0)
    for j in range(SINGLE):
        for g in range(8):
            block = send[ALONE + j, 4 * g : 4 * g + 4].reshape(8, 8, HIGH)
            z_out[j, :, 8 * g : 8 * g + 8, :] = jnp.swapaxes(block, 0, 1)
    lax.fori_loop(28, 32, lambda i, c: (exchange(0, 0, 2, *peer(i)).start(), c)[1], 0)
    def apart(j):
        for k in FAR:
            along_z(z_out.at[j], z_in.at[j], z_send.at[j], z_recv.at[j], k).start()
        z_in[j, z] = z_out[j, z]

    apart(0)
    apart(1)
    exchange_all(1, 2, 2)

    mask_copy.wait()
    level_copy.wait()
    distance = 100.0 + 2.0 * level_in[...]

    def cutoff(k):
        total = jnp.sum(mask_in[0, k : k + 1, :].astype(F32), axis=1, keepdims=True)
        return jnp.broadcast_to((total + 1.0) * 0.5, (8, HIGH))

    cut_y, cut_x = cutoff(0), cutoff(1)
    line = lax.broadcasted_iota(jnp.int32, (8, HIGH), 0)
    about = jnp.where(line == 0, distance, jnp.where(line == 1, cut_y, cut_x))
    par_out[...] = about
    par_in[z] = about
    shape = (8, 8, HIGH)

    def signed(k):
        return jnp.where(k < N // 2, k, k - N).astype(F32)

    def propagate(t, g, k_x, distance, cut_y, cut_x):
        k_y = signed(lax.broadcasted_iota(jnp.int32, shape, 0) + g * 8 + 32 * lax.broadcasted_iota(jnp.int32, shape, 2))
        f_y, f_x = k_y * (1.0 / N), k_x * (1.0 / N)
        square = f_y * f_y + f_x * f_x
        quarters = (-4.0 * distance[None]) * (square / (2.0 + jnp.sqrt(4.0 - square)))
        whole = jnp.floor(quarters + 0.5)
        v = (quarters - whole) * (0.5 * math.pi)
        quadrant = whole - 4.0 * jnp.floor(whole * 0.25)
        v2 = v * v
        sine = v + v * v2 * (-1.6666654611e-1 + v2 * (8.3321608736e-3 - v2 * 1.9515295891e-4))
        cosine = 1.0 - 0.5 * v2 + v2 * v2 * (4.166664568298827e-2 + v2 * (-1.388731625493765e-3 + v2 * 2.443315711809948e-5))
        odd = (quadrant == 1.0) | (quadrant == 3.0)
        re = jnp.where(odd, sine, cosine)
        im = jnp.where(odd, cosine, sine)
        inside = (jnp.abs(k_y) < cut_y[None]) & (jnp.abs(k_x) < cut_x[None])
        weight = jnp.where(inside, 1.0, 0.0)
        prop[t, pl.ds(g * 8, 8), 0] = jnp.where((quadrant == 1.0) | (quadrant == 2.0), -re, re) * weight
        prop[t, pl.ds(g * 8, 8), 1] = jnp.where(quadrant >= 2.0, -im, im) * weight

    def propagate_tile(i, c):
        t, g = i // 4, lax.rem(i, 4)
        k_x = signed(column + 32 * (t * 8 + lax.broadcasted_iota(jnp.int32, shape, 1)))
        propagate(t, g, k_x, distance, cut_y, cut_x)
        return c

    with jax.named_scope("H"):
        lax.fori_loop(0, 4 * ALONE, propagate_tile, 0)
    for k in FAR:
        along_z(par_out, par_in, all_send, all_recv, k, True).start()

    def prepare_alone():
        for k in FAR:
            for j in range(SINGLE):
                from_z(z_out.at[j], z_in.at[j], z_send.at[j], z_recv.at[j], k).wait_recv()
            from_z(par_out, par_in, all_send, all_recv, k, True).wait_recv()
        for j in range(SINGLE):
            for g in range(8):
                block = jnp.swapaxes(z_in[j, :, 8 * g : 8 * g + 8, :], 0, 1)
                send[ALONE + j, 4 * g : 4 * g + 4] = block.reshape(4, 2, 8, HIGH)
        each = [jnp.concatenate([par_in[p, j : j + 1, :] for p in range(8)]) for j in range(3)]

        def group(i, c):
            t = ALONE + i // 4
            k_x = signed(jnp.full(shape, column + 32 * (8 * t + z), jnp.int32))
            propagate(t, lax.rem(i, 4), k_x, *each)
            return c

        lax.fori_loop(0, 4 * SINGLE, group, 0)

    def height(t, c):
        re, im = joined(dft32(recv[t, :, 0], recv[t, :, 1], small, -1))
        cosine, sine = turn[0], turn[1]
        re, im = along_lanes(re * cosine + im * sine, im * cosine - re * sine, w, 0)
        p_re, p_im = prop[t, :, 0], prop[t, :, 1]
        re, im = along_lanes(re * p_re - im * p_im, re * p_im + im * p_re, w, 2)
        re, im = joined(dft32(re * cosine - im * sine, im * cosine + re * sine, small, 1))
        part[t, :, 0] = re
        part[t, :, 1] = im
        return c

    def height_alone(j):
        t = ALONE + j
        re, im = joined(dft32(recv[t, :, 0], recv[t, :, 1], small, -1))
        cosine, sine = turn[0], turn[1]
        re, im = along_lanes(re * cosine + im * sine, im * cosine - re * sine, w, 0)
        p_re, p_im = prop[t, :, 0], prop[t, :, 1]
        left = jnp.concatenate(
            [jnp.sum(re * p_re - im * p_im, axis=1), jnp.sum(re * p_im + im * p_re, axis=1)], axis=1
        )
        both = split_dot(left, w, 2)
        re, im = both[:, :HIGH], both[:, HIGH:]
        cosine, sine = flat[0], flat[1]
        right = jnp.concatenate([re * cosine - im * sine, im * cosine + re * sine])
        top = right.astype(BF16)
        rest = (right - top.astype(F32)).astype(BF16)
        dot = functools.partial(jnp.dot, preferred_element_type=F32)
        result = dot(short[0], top) + (dot(short[0], rest) + dot(short[1], top))
        sum_out[j] = result.reshape(Z, 8, HIGH)
        sum_in[j, z] = sum_out[j, z]
        for k in FAR:
            along_z(sum_out.at[j], sum_in.at[j], sum_send.at[j], sum_recv.at[j], k).start()

    def ring_copy(q, t0, n, step, source):
        tiles = pl.ds(t0, n)
        return pltpu.make_async_remote_copy(
            part.at[tiles, pl.ds(source * 4, 4)], ring.at[tiles, step], ring_send.at[q, step], ring_recv.at[q, step],
            device_id=(up if step < 4 else down, row), device_id_type=MESH,
        )

    def ring_step(q, t0, n, step):
        tiles = pl.ds(t0, n)
        lines = [(step, lax.rem(z + 4 - step, Z))] + ([(step + 4, lax.rem(z + 5 + step, Z))] if step < 3 else [])
        for i, source in lines:
            if step > 0:
                ring_copy(q, t0, n, i - 1, source).wait_recv()
                block = pl.ds(source * 4, 4)
                part[tiles, block] = part[tiles, block] + ring[tiles, i - 1]
        for i, source in lines:
            ring_copy(q, t0, n, i, source).start()

    def pair_copy(q):
        tiles = pl.ds(PAIRED[q], PAIRED[q + 1] - PAIRED[q])
        return pltpu.make_async_remote_copy(
            own.at[tiles, pl.ds(y_lo * 2, 2)], pair.at[tiles], pair_send.at[q], pair_recv.at[q],
            device_id=(other, mate), device_id_type=MESH,
        )

    def ring_end(q, t0, n):
        tiles = pl.ds(t0, n)
        ring_copy(q, t0, n, 6, z).wait_recv()
        ring_copy(q, t0, n, 3, z).wait_recv()
        own[tiles] = part[tiles, pl.ds(z * 4, 4)] + (ring[tiles, 3] + ring[tiles, 6])

    def chunk(q, t0, n, ahead, before=None, ended=None):
        with jax.named_scope("wait_a2a"):
            exchange_whole(q, t0, n).wait_recv()
        with jax.named_scope("C"):
            lax.fori_loop(t0, t0 + n, height, 0)
        ring_step(q, t0, n, 0)
        ahead()
        if before is not None:
            ring_step(*before, 2)
        if ended is not None:
            ring_end(*ended)
        with jax.named_scope("ring"):
            ring_step(q, t0, n, 1)
            if before is not None:
                ring_step(*before, 3)

    keep = 2 - 2 * y_lo

    def deliver(half, to):
        return pltpu.make_async_remote_copy(
            final.at[half, to], final_in.at[half, column], final_send.at[half], final_recv.at[half],
            device_id=(other, to), device_id_type=MESH,
        )

    def deliver_whole(half):
        return pltpu.make_async_remote_copy(
            final.at[half], final_in.at[half], final_send.at[half], final_recv.at[half],
            device_id=(other, row), device_id_type=MESH,
        )

    def hand_over(half):
        tiles = pl.ds(half * 8, 8)
        for a in range(2):
            block = [(own[tiles, keep + a, k] + pair[tiles, a, k]).reshape(64, HIGH) for k in range(2)]
            final[half, a * 16 : a * 16 + 16] = jnp.concatenate(block).T.reshape(16, 8, HIGH)

    def dispatch(half):
        for to, _ in far_first:
            deliver(half, to).start()

    chunk(0, 0, 2, lambda: exchange_all(2, 4, 2))

    def second():
        exchange_all(3, 6, 2)
        apart(2)
        apart(3)

    chunk(1, 2, 2, second, (0, 0, 2))

    def middle(q, c):
        def ahead():
            @pl.when(q < WIDE - 2)
            def _():
                exchange_all(q + 2, 2 * q + 4, 2)

            @pl.when(q >= WIDE - 2)
            def _():
                for j in range(2):
                    i = 2 * (q + 2 - WIDE) + j
                    exchange_all(WIDE + i, ALONE + i, 1)

            @pl.when(q == 3)
            def _():
                prepare_alone()

        chunk(q, 2 * q, 2, ahead, (q - 1, 2 * q - 2, 2), (q - 2, 2 * q - 4, 2))
        return c

    lax.fori_loop(2, WIDE, middle, 0)
    def single(j):
        with jax.named_scope("wait_alone"):
            exchange_whole(WIDE + j, ALONE + j, 1).wait_recv()
        if j == SINGLE - 1:
            pair_copy(0).start()
            pair_copy(1).start()
        with jax.named_scope("C_alone"):
            height_alone(j)

    def summed(j):
        for k in FAR:
            from_z(sum_out.at[j], sum_in.at[j], sum_send.at[j], sum_recv.at[j], k).wait_recv()
        lines = jnp.swapaxes(sum_in[j], 0, 1)
        for k in range(2):
            own[ALONE + j, :, k] = lines[4 * k : 4 * k + 4]

    single(0)
    with jax.named_scope("ring2"):
        ring_end(WIDE - 2, ALONE - 4, 2)
        ring_step(WIDE - 1, ALONE - 2, 2, 2)
    single(1)
    with jax.named_scope("ring3"):
        ring_step(WIDE - 1, ALONE - 2, 2, 3)
        summed(0)
    single(2)
    with jax.named_scope("ring_end"):
        ring_end(WIDE - 1, ALONE - 2, 2)
        summed(1)
        summed(2)
    single(3)
    with jax.named_scope("pair0"):
        pair_copy(0).wait_recv()
        hand_over(0)
    with jax.named_scope("sums"):
        summed(3)
        pair_copy(2).start()
    dispatch(0)
    with jax.named_scope("pair1"):
        pair_copy(1).wait_recv()
        pair_copy(2).wait_recv()
    with jax.named_scope("pack1"):
        hand_over(1)
    dispatch(1)

    def settle(q, c):
        exchange_whole(q, 2 * q, 2).wait_send()
        for step in range(7):
            ring_copy(q, 2 * q, 2, step, z).wait_send()
        return c

    lax.fori_loop(0, WIDE, settle, 0)
    for q in range(3):
        pair_copy(q).wait_send()
    for j in range(SINGLE):
        exchange_whole(WIDE + j, ALONE + j, 1).wait_send()
        for k in FAR:
            along_z(z_out.at[j], z_in.at[j], z_send.at[j], z_recv.at[j], k).wait_send()
            along_z(sum_out.at[j], sum_in.at[j], sum_send.at[j], sum_recv.at[j], k).wait_send()
    for k in FAR:
        along_z(par_out, par_in, all_send, all_recv, k, True).wait_send()
    deliver_whole(0).wait_recv()
    both = split_dot(final_in[0].reshape(8 * LOW, HIGH), w, 4, slice(0, HIGH))
    with jax.named_scope("final_wait"):
        deliver_whole(1).wait_recv()
    both = both + split_dot(final_in[1].reshape(8 * LOW, HIGH), w, 4, slice(HIGH, 2 * HIGH))
    re, im = both[:, :HIGH].reshape(LOW, 8, HIGH), both[:, HIGH:].reshape(LOW, 8, HIGH)
    cosine, sine = turn[0] * 0.25, turn[1] * 0.25
    pieces = dft32(re * cosine - im * sine, im * cosine + re * sine, small, 1)
    for k in range(8):
        for j in range(4):
            lanes = pl.ds((k * 4 + j) * HIGH, HIGH)
            out_ref[0, :, lanes] = pieces[k][0][j]
            out_ref[1, :, lanes] = pieces[k][1][j]
    deliver_whole(0).wait_send()
    deliver_whole(1).wait_send()


def local(target, depth_index, band_mask):
    turn, small, matrices, flat, short = tables()
    anywhere = pl.BlockSpec(memory_space=pl.ANY)
    dma = pltpu.SemaphoreType.DMA
    return pl.pallas_call(
        kernel,
        out_shape=pltpu.VMEM((2, 8, N), F32),
        in_specs=[anywhere] * 8,
        out_specs=pl.BlockSpec(memory_space=pltpu.VMEM),
        scratch_shapes=[
            pltpu.VMEM((2, HIGH, N), F32),
            pltpu.VMEM((LOW, 2, HIGH, HIGH), F32),
            pltpu.VMEM((TILES, LOW, 2, 8, HIGH), F32),
            pltpu.VMEM((TILES, LOW, 2, 8, HIGH), F32),
            pltpu.VMEM((TILES, LOW, 2, 8, HIGH), F32),
            pltpu.VMEM((TILES, LOW, 2, 8, HIGH), F32),
            pltpu.VMEM((ALONE, 7, 4, 2, 8, HIGH), F32),
            pltpu.VMEM((TILES, 4, 2, 8, HIGH), F32),
            pltpu.VMEM((TILES, 2, 2, 8, HIGH), F32),
            pltpu.VMEM((2, LOW, 8, HIGH), F32),
            pltpu.VMEM((2, LOW, 8, HIGH), F32),
            pltpu.VMEM((1, 2, N), jnp.int32),
            pltpu.SMEM((1,), jnp.int32),
            pltpu.VMEM((8, HIGH), F32),
            pltpu.VMEM((8, HIGH), F32),
            pltpu.VMEM(turn.shape, F32),
            pltpu.VMEM(small.shape, F32),
            pltpu.VMEM(matrices.shape, BF16),
            pltpu.VMEM(flat.shape, F32),
            pltpu.VMEM(short.shape, BF16),
            pltpu.VMEM((SINGLE, Z, 2 * LOW, HIGH), F32),
            pltpu.VMEM((SINGLE, Z, 2 * LOW, HIGH), F32),
            pltpu.VMEM((8, HIGH), F32),
            pltpu.VMEM((Z, 8, HIGH), F32),
            pltpu.VMEM((SINGLE, Z, 8, HIGH), F32),
            pltpu.VMEM((SINGLE, Z, 8, HIGH), F32),
            dma((4,)),
            dma((6,)),
            dma((CHUNKS,)),
            dma((CHUNKS,)),
            dma((WIDE, 7)),
            dma((WIDE, 7)),
            dma((3,)),
            dma((3,)),
            dma((2,)),
            dma((2,)),
            dma((2,)),
            dma((2,)),
            dma((SINGLE, Z)),
            dma((SINGLE, Z)),
            dma((Z,)),
            dma((Z,)),
            dma((SINGLE, Z)),
            dma((SINGLE, Z)),
        ],
        compiler_params=pltpu.CompilerParams(
            collective_id=0, has_side_effects=True, vmem_limit_bytes=60 * 1024 * 1024
        ),
        name="hologram",
    )(target, band_mask, depth_index, turn, small, matrices, flat, short)


def solution(mesh):
    in_specs = (P("depth", None, "rows", None), P("depth"), P("depth", None, None))
    out_specs = P(None, ("depth", "rows"), None)
    return jax.shard_map(local, mesh=mesh, in_specs=in_specs, out_specs=out_specs, check_vma=False)
```

```python
import functools
import math

import jax
import jax.numpy as jnp
import ml_dtypes
import numpy as np
from jax import lax
from jax.experimental import pallas as pl
from jax.experimental.pallas import tpu as pltpu
from jax.sharding import PartitionSpec as P

MESH = pl.DeviceIdType.MESH
N = 4096
LOW = 32
HIGH = 128
Z = 8
TILES = 16
WIDE = 6
SINGLE = 4
CHUNKS = WIDE + SINGLE
ALONE = 2 * WIDE
PAIRED = (0, 8, 15)
FAR = (4, 3, 5, 2, 6, 1, 7)
F32 = jnp.float32
BF16 = jnp.bfloat16


def tables():
    angle = 2.0 * np.pi / N * np.outer(np.arange(LOW), np.arange(HIGH))
    turn = np.stack([np.cos(angle), np.sin(angle)]) / 64.0
    turn = np.broadcast_to(turn[:, :, None, :], (2, LOW, 8, HIGH)).astype(np.float32)
    angle = 2.0 * np.pi / LOW * np.outer(np.arange(1, 4), np.arange(8))
    small = np.stack([np.cos(angle), np.sin(angle)])
    small = np.broadcast_to(small[:, :, :, None, None], (2, 3, 8, 8, HIGH)).astype(np.float32)
    angle = 2.0 * np.pi / HIGH * (np.outer(np.arange(HIGH), np.arange(HIGH)) % HIGH)
    cosine, sine = np.cos(angle), np.sin(angle)
    ahead = np.block([[cosine, -sine], [sine, cosine]])
    parts = []
    for matrix in (ahead, ahead.T):
        top = matrix.astype(np.float32).astype(ml_dtypes.bfloat16)
        rest = (matrix - top.astype(np.float64)).astype(np.float32).astype(ml_dtypes.bfloat16)
        parts += [top, rest]
    order = np.arange(256).reshape(2, 2, 64).swapaxes(0, 1).reshape(256)
    parts += [parts[2][order], parts[3][order]]
    angle = 2.0 * np.pi / LOW * np.outer(np.arange(LOW), np.arange(LOW))
    cosine, sine = np.cos(angle), np.sin(angle)
    short = np.block([[cosine, -sine], [sine, cosine]])
    short = short.reshape(2, Z, 4, 2 * LOW).swapaxes(0, 1).reshape(2 * LOW, 2 * LOW)
    top = short.astype(np.float32).astype(ml_dtypes.bfloat16)
    rest = (short - top.astype(np.float64)).astype(np.float32).astype(ml_dtypes.bfloat16)
    return turn, small, np.stack(parts), turn[:, :, 0, :].copy(), np.stack([top, rest])


def dft4(a, sign):
    (r0, i0), (r1, i1), (r2, i2), (r3, i3) = a
    s0r, s0i, d0r, d0i = r0 + r2, i0 + i2, r0 - r2, i0 - i2
    s1r, s1i, d1r, d1i = r1 + r3, i1 + i3, r1 - r3, i1 - i3
    up, down = (d0r - d1i, d0i + d1r), (d0r + d1i, d0i - d1r)
    first, third = (up, down) if sign > 0 else (down, up)
    return [(s0r + s1r, s0i + s1i), first, (s0r - s1r, s0i - s1i), third]


def dft32(re, im, small_ref, sign):
    half = math.sqrt(0.5)
    columns = dft4([(re[8 * n : 8 * n + 8], im[8 * n : 8 * n + 8]) for n in range(4)], sign)
    turned = [columns[0]]
    for k in range(1, 4):
        r, i = columns[k]
        c, s = small_ref[0, k - 1], small_ref[1, k - 1]
        turned.append((r * c + i * s, i * c - r * s) if sign < 0 else (r * c - i * s, i * c + r * s))
    re = jnp.stack([t[0] for t in turned])
    im = jnp.stack([t[1] for t in turned])
    rows = [(re[:, n], im[:, n]) for n in range(8)]
    even = dft4(rows[0::2], sign)
    odd = dft4(rows[1::2], sign)
    (r1, i1), (r2, i2), (r3, i3) = odd[1:]
    if sign < 0:
        odd = [odd[0], ((r1 + i1) * half, (i1 - r1) * half), (i2, -r2), ((i3 - r3) * half, (-r3 - i3) * half)]
    else:
        odd = [odd[0], ((r1 - i1) * half, (i1 + r1) * half), (-i2, r2), ((-r3 - i3) * half, (r3 - i3) * half)]
    result = [(e[0] + o[0], e[1] + o[1]) for e, o in zip(even, odd)]
    return result + [(e[0] - o[0], e[1] - o[1]) for e, o in zip(even, odd)]


def joined(pieces):
    return jnp.concatenate([p[0] for p in pieces]), jnp.concatenate([p[1] for p in pieces])


def split_dot(left, w_ref, which, rows=slice(None)):
    top = left.astype(BF16)
    rest = (left - top.astype(F32)).astype(BF16)
    w_top, w_rest = w_ref[which, rows], w_ref[which + 1, rows]
    dot = functools.partial(jnp.dot, preferred_element_type=F32)
    return dot(top, w_top) + (dot(rest, w_top) + dot(top, w_rest))


def along_lanes(re, im, w_ref, which):
    left = jnp.concatenate([re.reshape(8 * LOW, HIGH), im.reshape(8 * LOW, HIGH)], axis=1)
    result = split_dot(left, w_ref, which)
    return result[:, :HIGH].reshape(LOW, 8, HIGH), result[:, HIGH:].reshape(LOW, 8, HIGH)


def kernel(
    x_ref, mask_ref, level_ref, turn_ref, small_ref, w_ref, flat_ref, short_ref, out_ref,
    xbuf, tbuf, send, recv, prop, part, ring, own, pair, final, final_in, mask_in, level_at, level_out, level_in,
    turn, small, w, flat, short, z_out, z_in, par_out, par_in, sum_out, sum_in, mate_in, mate_own,
    x_sem, in_sem, send_sem, recv_sem, ring_send, ring_recv, pair_send, pair_recv, final_send, final_recv,
    par_send, par_recv, z_send, z_recv, all_send, all_recv, sum_send, sum_recv, mate_send, mate_recv,
):
    depth = lax.axis_index("depth")
    row = lax.axis_index("rows")
    z, y_lo = depth // 2, lax.rem(depth, 2)
    core, y_hi, x = lax.rem(row, 2), lax.rem(row // 2, 4), row // 8
    other = depth + 1 - 2 * y_lo
    up, down = lax.rem(depth + 2, 2 * Z), lax.rem(depth + 2 * Z - 2, 2 * Z)

    column = (x * 4 + lax.rem(y_hi + y_lo * core, 4)) * 2 + core
    mate = (x * 4 + lax.rem(y_hi + core * (3 - 2 * y_lo), 4)) * 2 + core

    def place(to_x, to_y, to_core):
        return (to_x * 4 + to_y) * 2 + to_core, (to_x * 4 + lax.rem(to_y + to_core * (1 - y_lo), 4)) * 2 + to_core

    def peer(i):
        h = lax.rem(i, 4)
        to_y = lax.rem(y_hi + lax.rem(h, 2) * 2 + h // 2, 4)
        to_core = lax.rem(core + lax.rem(i // 4, 2), 2)
        to_x = lax.rem(x + i // 8, 4)
        return place(to_x, to_y, to_core)

    xs = [lax.rem(x + k, 4) for k in range(4)]
    ys = [lax.rem(y_hi + y_lo + k, 4) for k in range(4)]
    cores = [core, 1 - core]
    near_first = [place(xs[i], ys[h], c) for i in range(4) for c in cores for h in (1, 2, 0, 3)]
    far_first = [place(xs[i], ys[h], c) for i in (2, 1, 3, 0) for h in (1, 2, 0, 3) for c in cores]

    def load(g):
        rows = pl.ds(pl.multiple_of(g * 32, 32), 32)
        return pltpu.make_async_copy(x_ref.at[0, :, rows, :], xbuf.at[:, rows, :], x_sem.at[g])

    load_small = pltpu.make_async_copy(small_ref, small, in_sem.at[0])
    load_turn = pltpu.make_async_copy(turn_ref, turn, in_sem.at[1])
    load_w = pltpu.make_async_copy(w_ref, w, in_sem.at[2])
    load_level = pltpu.make_async_copy(level_ref, level_at, in_sem.at[3])
    load_small.start()
    load(0).start()
    load_turn.start()
    for g in range(1, 4):
        load(g).start()
    load_w.start()
    load_level.start()
    load_flat = pltpu.make_async_copy(flat_ref, flat, in_sem.at[4])
    load_short = pltpu.make_async_copy(short_ref, short, in_sem.at[5])
    load_flat.start()
    load_short.start()

    barrier = pltpu.get_barrier_semaphore()

    with jax.named_scope("greet"):
        for to in [(other, r) for r, _ in far_first] + [(2 * lax.rem(z + k, Z) + y_lo, row) for k in FAR] + [
            (2 * lax.rem(z + k, Z) + 1 - y_lo, mate) for k in FAR
        ]:
            pl.semaphore_signal(barrier, inc=1, device_id=to, device_id_type=MESH)

    load_small.wait()
    load_turn.wait()

    def width_first(t, c):
        rows = pl.ds(pl.multiple_of(t * 8, 8), 8)
        cells = [jnp.stack([xbuf[k, rows, a * HIGH : (a + 1) * HIGH] for a in range(LOW)]) for k in range(2)]
        re, im = joined(dft32(cells[0], cells[1], small, -1))
        cosine, sine = turn[0], turn[1]
        tbuf[:, 0, rows, :] = re * cosine + im * sine
        tbuf[:, 1, rows, :] = im * cosine - re * sine
        return c

    def width_group(g, c):
        load(g).wait()
        return lax.fori_loop(g * 4, g * 4 + 4, width_first, c)

    with jax.named_scope("A1"):
        lax.fori_loop(0, 4, width_group, 0)

    load_level.wait()
    level_out[...] = jnp.full((8, HIGH), level_at[0].astype(F32))
    load_w.wait()
    load_flat.wait()
    load_short.wait()
    with jax.named_scope("barrier"):
        pl.semaphore_wait(barrier, 46)
    mask_copy = pltpu.make_async_remote_copy(
        mask_ref, mask_in, par_send.at[0], par_recv.at[0], device_id=(other, row), device_id_type=MESH
    )
    level_copy = pltpu.make_async_remote_copy(
        level_out, level_in, par_send.at[1], par_recv.at[1], device_id=(other, row), device_id_type=MESH
    )
    mask_copy.start()
    level_copy.start()

    def exchange(q, t0, n, to, block):
        tiles = pl.ds(t0, n)
        return pltpu.make_async_remote_copy(
            send.at[tiles, block], recv.at[tiles, row], send_sem, recv_sem.at[q],
            device_id=(other, to), device_id_type=MESH,
        )

    def exchange_whole(q, t0, n):
        tiles = pl.ds(t0, n)
        return pltpu.make_async_remote_copy(
            send.at[tiles], recv.at[tiles], send_sem, recv_sem.at[q],
            device_id=(other, row), device_id_type=MESH,
        )

    def exchange_all(q, t0, n):
        for to, block in near_first:
            exchange(q, t0, n, to, block).start()

    def along_z(out, into, send_sem, recv_sem, k, shared=False):
        to = lax.rem(z + k, Z)
        return pltpu.make_async_remote_copy(
            out if shared else out.at[to], into.at[z], send_sem, recv_sem,
            device_id=(2 * to + y_lo, row), device_id_type=MESH,
        )

    def amount(buffer, send_sem, recv_sem):
        return pltpu.make_async_remote_copy(
            buffer, buffer, send_sem, recv_sem, device_id=(other, row), device_id_type=MESH
        )

    seven = pl.ds(0, Z - 1)
    all_z = amount(z_in.at[:, seven], z_send, z_recv)
    all_par = amount(par_in.at[seven], all_send, all_recv)
    all_mate = amount(mate_in, mate_send, mate_recv)

    def width_last(g, c):
        @pl.when(g > 0)
        def _():
            for h in range(4):
                exchange(0, 0, 2, *peer((g - 1) * 4 + h)).start()

        for h in range(4):
            _, block = peer(g * 4 + h)
            both = split_dot(jnp.concatenate([tbuf[block, 0], tbuf[block, 1]], axis=1), w, 0)
            for k in range(2):
                send[:, block, k] = both[:, k * HIGH : (k + 1) * HIGH].T.reshape(TILES, 8, HIGH)
        return c

    with jax.named_scope("A2"):
        lax.fori_loop(0, 8, width_last, 0)
    for j in range(SINGLE):
        for g in range(8):
            block = send[ALONE + j, 4 * g : 4 * g + 4].reshape(8, 8, HIGH)
            z_out[j, :, 8 * g : 8 * g + 8, :] = jnp.swapaxes(block, 0, 1)
    lax.fori_loop(28, 32, lambda i, c: (exchange(0, 0, 2, *peer(i)).start(), c)[1], 0)
    def apart(j):
        for k in FAR:
            along_z(z_out.at[j], z_in.at[j], z_send, z_recv, k).start()
        z_in[j, z] = z_out[j, z]

    apart(0)
    apart(1)
    exchange_all(1, 2, 2)

    mask_copy.wait()
    level_copy.wait()
    distance = 100.0 + 2.0 * level_in[...]

    def cutoff(k):
        total = jnp.sum(mask_in[0, k : k + 1, :].astype(F32), axis=1, keepdims=True)
        return jnp.broadcast_to((total + 1.0) * 0.5, (8, HIGH))

    cut_y, cut_x = cutoff(0), cutoff(1)
    line = lax.broadcasted_iota(jnp.int32, (8, HIGH), 0)
    about = jnp.where(line == 0, distance, jnp.where(line == 1, cut_y, cut_x))
    par_out[...] = about
    par_in[z] = about
    shape = (8, 8, HIGH)

    def signed(k):
        return jnp.where(k < N // 2, k, k - N).astype(F32)

    def propagate(t, g, k_x, distance, cut_y, cut_x):
        k_y = signed(lax.broadcasted_iota(jnp.int32, shape, 0) + g * 8 + 32 * lax.broadcasted_iota(jnp.int32, shape, 2))
        f_y, f_x = k_y * (1.0 / N), k_x * (1.0 / N)
        square = f_y * f_y + f_x * f_x
        quarters = (-4.0 * distance[None]) * (square / (2.0 + jnp.sqrt(4.0 - square)))
        whole = jnp.floor(quarters + 0.5)
        v = (quarters - whole) * (0.5 * math.pi)
        quadrant = whole - 4.0 * jnp.floor(whole * 0.25)
        v2 = v * v
        sine = v + v * v2 * (-1.6666654611e-1 + v2 * (8.3321608736e-3 - v2 * 1.9515295891e-4))
        cosine = 1.0 - 0.5 * v2 + v2 * v2 * (4.166664568298827e-2 + v2 * (-1.388731625493765e-3 + v2 * 2.443315711809948e-5))
        odd = (quadrant == 1.0) | (quadrant == 3.0)
        re = jnp.where(odd, sine, cosine)
        im = jnp.where(odd, cosine, sine)
        inside = (jnp.abs(k_y) < cut_y[None]) & (jnp.abs(k_x) < cut_x[None])
        weight = jnp.where(inside, 1.0, 0.0)
        prop[t, pl.ds(g * 8, 8), 0] = jnp.where((quadrant == 1.0) | (quadrant == 2.0), -re, re) * weight
        prop[t, pl.ds(g * 8, 8), 1] = jnp.where(quadrant >= 2.0, -im, im) * weight

    def propagate_tile(i, c):
        t, g = i // 4, lax.rem(i, 4)
        k_x = signed(column + 32 * (t * 8 + lax.broadcasted_iota(jnp.int32, shape, 1)))
        propagate(t, g, k_x, distance, cut_y, cut_x)
        return c

    with jax.named_scope("H"):
        lax.fori_loop(0, 4 * ALONE, propagate_tile, 0)
    for k in FAR:
        along_z(par_out, par_in, all_send, all_recv, k, True).start()

    def prepare_alone():
        all_z.wait_recv()
        all_par.wait_recv()
        for j in range(SINGLE):
            for g in range(8):
                block = jnp.swapaxes(z_in[j, :, 8 * g : 8 * g + 8, :], 0, 1)
                send[ALONE + j, 4 * g : 4 * g + 4] = block.reshape(4, 2, 8, HIGH)
        each = [jnp.concatenate([par_in[p, j : j + 1, :] for p in range(8)]) for j in range(3)]

        def group(i, c):
            t = ALONE + i // 4
            k_x = signed(jnp.full(shape, column + 32 * (8 * t + z), jnp.int32))
            propagate(t, lax.rem(i, 4), k_x, *each)
            return c

        lax.fori_loop(0, 4 * SINGLE, group, 0)

    def height(t, c):
        re, im = joined(dft32(recv[t, :, 0], recv[t, :, 1], small, -1))
        cosine, sine = turn[0], turn[1]
        re, im = along_lanes(re * cosine + im * sine, im * cosine - re * sine, w, 0)
        p_re, p_im = prop[t, :, 0], prop[t, :, 1]
        re, im = along_lanes(re * p_re - im * p_im, re * p_im + im * p_re, w, 2)
        re, im = joined(dft32(re * cosine - im * sine, im * cosine + re * sine, small, 1))
        part[t, :, 0] = re
        part[t, :, 1] = im
        return c

    def to_mate(k):
        to = lax.rem(z + k, Z)
        return pltpu.make_async_remote_copy(
            sum_out.at[SINGLE - 1, to], mate_in.at[z], mate_send, mate_recv,
            device_id=(2 * to + 1 - y_lo, mate), device_id_type=MESH,
        )

    def height_alone(j):
        t = ALONE + j
        re, im = joined(dft32(recv[t, :, 0], recv[t, :, 1], small, -1))
        cosine, sine = turn[0], turn[1]
        re, im = along_lanes(re * cosine + im * sine, im * cosine - re * sine, w, 0)
        p_re, p_im = prop[t, :, 0], prop[t, :, 1]
        left = jnp.concatenate(
            [jnp.sum(re * p_re - im * p_im, axis=1), jnp.sum(re * p_im + im * p_re, axis=1)], axis=1
        )
        both = split_dot(left, w, 2)
        re, im = both[:, :HIGH], both[:, HIGH:]
        cosine, sine = flat[0], flat[1]
        right = jnp.concatenate([re * cosine - im * sine, im * cosine + re * sine])
        top = right.astype(BF16)
        rest = (right - top.astype(F32)).astype(BF16)
        dot = functools.partial(jnp.dot, preferred_element_type=F32)
        result = dot(short[0], top) + (dot(short[0], rest) + dot(short[1], top))
        sum_out[j] = result.reshape(Z, 8, HIGH)
        sum_in[j, z] = sum_out[j, z]
        if j == SINGLE - 1:
            for k in FAR + (0,):
                to_mate(k).start()
        for k in FAR:
            along_z(sum_out.at[j], sum_in.at[j], sum_send, sum_recv.at[j], k).start()

    def ring_copy(q, t0, n, step, source):
        tiles = pl.ds(t0, n)
        return pltpu.make_async_remote_copy(
            part.at[tiles, pl.ds(source * 4, 4)], ring.at[tiles, step], ring_send,
            ring_recv.at[q, {4: 0, 5: 1, 6: 3}.get(step, step)],
            device_id=(up if step < 4 else down, row), device_id_type=MESH,
        )

    def ring_wait(q, t0, n, step):
        blocks = ring.at[pl.ds(t0, n), pl.ds(0, 1 if step == 2 else 2)]
        amount(blocks, ring_send, ring_recv.at[q, step]).wait_recv()

    def ring_step(q, t0, n, step):
        tiles = pl.ds(t0, n)
        lines = [(step, lax.rem(z + 4 - step, Z))] + ([(step + 4, lax.rem(z + 5 + step, Z))] if step < 3 else [])
        if step > 0:
            ring_wait(q, t0, n, step - 1)
        for i, source in lines:
            if step > 0:
                block = pl.ds(source * 4, 4)
                part[tiles, block] = part[tiles, block] + ring[tiles, i - 1]
        for i, source in lines:
            ring_copy(q, t0, n, i, source).start()

    def pair_copy(q):
        tiles = pl.ds(PAIRED[q], PAIRED[q + 1] - PAIRED[q])
        return pltpu.make_async_remote_copy(
            own.at[tiles, pl.ds(y_lo * 2, 2)], pair.at[tiles], pair_send.at[q], pair_recv.at[q],
            device_id=(other, mate), device_id_type=MESH,
        )

    def ring_end(q, t0, n):
        tiles = pl.ds(t0, n)
        ring_wait(q, t0, n, 3)
        own[tiles] = part[tiles, pl.ds(z * 4, 4)] + (ring[tiles, 3] + ring[tiles, 6])

    def chunk(q, t0, n, ahead, before=None, ended=None):
        with jax.named_scope("wait_a2a"):
            exchange_whole(q, t0, n).wait_recv()
        with jax.named_scope("C"):
            lax.fori_loop(t0, t0 + n, height, 0)
        ring_step(q, t0, n, 0)
        ahead()
        if before is not None:
            ring_step(*before, 2)
        if ended is not None:
            ring_end(*ended)
        with jax.named_scope("ring"):
            ring_step(q, t0, n, 1)
            if before is not None:
                ring_step(*before, 3)

    keep = 2 - 2 * y_lo

    def deliver(half, to):
        return pltpu.make_async_remote_copy(
            final.at[half, to], final_in.at[half, column], final_send, final_recv.at[half],
            device_id=(other, to), device_id_type=MESH,
        )

    def deliver_whole(half):
        return pltpu.make_async_remote_copy(
            final.at[half], final_in.at[half], final_send, final_recv.at[half],
            device_id=(other, row), device_id_type=MESH,
        )

    def hand_over(half):
        tiles = pl.ds(half * 8, 8)
        for a in range(2):
            block = [(own[tiles, keep + a, k] + pair[tiles, a, k]).reshape(64, HIGH) for k in range(2)]
            final[half, a * 16 : a * 16 + 16] = jnp.concatenate(block).T.reshape(16, 8, HIGH)

    def dispatch(half):
        for to, _ in far_first:
            deliver(half, to).start()

    chunk(0, 0, 2, lambda: exchange_all(2, 4, 2))

    def second():
        exchange_all(3, 6, 2)
        apart(2)
        apart(3)

    chunk(1, 2, 2, second, (0, 0, 2))

    def middle(q, c):
        def ahead():
            @pl.when(q < WIDE - 2)
            def _():
                exchange_all(q + 2, 2 * q + 4, 2)

            @pl.when(q >= WIDE - 2)
            def _():
                for j in range(2):
                    i = 2 * (q + 2 - WIDE) + j
                    exchange_all(WIDE + i, ALONE + i, 1)

            @pl.when(q == 3)
            def _():
                prepare_alone()

        chunk(q, 2 * q, 2, ahead, (q - 1, 2 * q - 2, 2), (q - 2, 2 * q - 4, 2))
        return c

    lax.fori_loop(2, WIDE, middle, 0)
    def single(j):
        with jax.named_scope("wait_alone"):
            exchange_whole(WIDE + j, ALONE + j, 1).wait_recv()
        if j == SINGLE - 2:
            pair_copy(0).start()
        with jax.named_scope("C_alone"):
            height_alone(j)

    def summed(j):
        amount(sum_in.at[j, seven], sum_send, sum_recv.at[j]).wait_recv()
        lines = jnp.swapaxes(sum_in[j], 0, 1)
        for k in range(2):
            own[ALONE + j, :, k] = lines[4 * k : 4 * k + 4]

    single(0)
    with jax.named_scope("ring2"):
        ring_end(WIDE - 2, ALONE - 4, 2)
        ring_step(WIDE - 1, ALONE - 2, 2, 2)
    single(1)
    with jax.named_scope("ring3"):
        ring_step(WIDE - 1, ALONE - 2, 2, 3)
        summed(0)
    single(2)
    with jax.named_scope("ring_end"):
        ring_end(WIDE - 1, ALONE - 2, 2)
        summed(1)
    with jax.named_scope("pair0"):
        pair_copy(0).wait_recv()
        hand_over(0)
    single(3)
    with jax.named_scope("dispatch0"):
        summed(2)
        pair_copy(1).start()
        dispatch(0)
    with jax.named_scope("sums"):
        summed(SINGLE - 1)
        all_mate.wait_recv()
        lines = jnp.swapaxes(mate_in[...], 0, 1)
        for k in range(2):
            mate_own[:, k] = lines[4 * k : 4 * k + 4]
        pair[TILES - 1] = mate_own[pl.ds(keep, 2)]
    with jax.named_scope("pair1"):
        pair_copy(1).wait_recv()
    with jax.named_scope("pack1"):
        hand_over(1)
    with jax.named_scope("dispatch1"):
        dispatch(1)

    amount(send, send_sem, recv_sem.at[0]).wait_send()
    amount(ring, ring_send, ring_recv.at[0, 0]).wait_send()
    for q in range(2):
        pair_copy(q).wait_send()
    all_z.wait_send()
    all_par.wait_send()
    all_mate.wait_send()
    amount(sum_in.at[:, seven], sum_send, sum_recv.at[0]).wait_send()
    with jax.named_scope('final_wait0'):
        deliver_whole(0).wait_recv()
    both = split_dot(final_in[0].reshape(8 * LOW, HIGH), w, 4, slice(0, HIGH))
    with jax.named_scope("final_wait"):
        deliver_whole(1).wait_recv()
    both = both + split_dot(final_in[1].reshape(8 * LOW, HIGH), w, 4, slice(HIGH, 2 * HIGH))
    re, im = both[:, :HIGH].reshape(LOW, 8, HIGH), both[:, HIGH:].reshape(LOW, 8, HIGH)
    cosine, sine = turn[0] * 0.25, turn[1] * 0.25
    pieces = dft32(re * cosine - im * sine, im * cosine + re * sine, small, 1)
    for k in range(8):
        for j in range(4):
            lanes = pl.ds((k * 4 + j) * HIGH, HIGH)
            out_ref[0, :, lanes] = pieces[k][0][j]
            out_ref[1, :, lanes] = pieces[k][1][j]
    with jax.named_scope("last_sends"):
        amount(final, final_send, final_recv.at[0]).wait_send()


def local(target, depth_index, band_mask):
    turn, small, matrices, flat, short = tables()
    anywhere = pl.BlockSpec(memory_space=pl.ANY)
    dma = pltpu.SemaphoreType.DMA
    return pl.pallas_call(
        kernel,
        out_shape=pltpu.VMEM((2, 8, N), F32),
        in_specs=[anywhere] * 2 + [pl.BlockSpec(memory_space=pltpu.HBM)] + [anywhere] * 5,
        out_specs=pl.BlockSpec(memory_space=pltpu.VMEM),
        scratch_shapes=[
            pltpu.VMEM((2, HIGH, N), F32),
            pltpu.VMEM((LOW, 2, HIGH, HIGH), F32),
            pltpu.VMEM((TILES, LOW, 2, 8, HIGH), F32),
            pltpu.VMEM((TILES, LOW, 2, 8, HIGH), F32),
            pltpu.VMEM((TILES, LOW, 2, 8, HIGH), F32),
            pltpu.VMEM((TILES, LOW, 2, 8, HIGH), F32),
            pltpu.VMEM((ALONE, 7, 4, 2, 8, HIGH), F32),
            pltpu.VMEM((TILES, 4, 2, 8, HIGH), F32),
            pltpu.VMEM((TILES, 2, 2, 8, HIGH), F32),
            pltpu.VMEM((2, LOW, 8, HIGH), F32),
            pltpu.VMEM((2, LOW, 8, HIGH), F32),
            pltpu.VMEM((1, 2, N), jnp.int32),
            pltpu.SMEM((1,), jnp.int32),
            pltpu.VMEM((8, HIGH), F32),
            pltpu.VMEM((8, HIGH), F32),
            pltpu.VMEM(turn.shape, F32),
            pltpu.VMEM(small.shape, F32),
            pltpu.VMEM(matrices.shape, BF16),
            pltpu.VMEM(flat.shape, F32),
            pltpu.VMEM(short.shape, BF16),
            pltpu.VMEM((SINGLE, Z, 2 * LOW, HIGH), F32),
            pltpu.VMEM((SINGLE, Z, 2 * LOW, HIGH), F32),
            pltpu.VMEM((8, HIGH), F32),
            pltpu.VMEM((Z, 8, HIGH), F32),
            pltpu.VMEM((SINGLE, Z, 8, HIGH), F32),
            pltpu.VMEM((SINGLE, Z, 8, HIGH), F32),
            pltpu.VMEM((Z, 8, HIGH), F32),
            pltpu.VMEM((4, 2, 8, HIGH), F32),
            dma((4,)),
            dma((6,)),
            dma,
            dma((CHUNKS,)),
            dma,
            dma((WIDE, 4)),
            dma((2,)),
            dma((2,)),
            dma,
            dma((2,)),
            dma((2,)),
            dma((2,)),
            dma,
            dma,
            dma,
            dma,
            dma,
            dma((SINGLE,)),
            dma,
            dma,
        ],
        compiler_params=pltpu.CompilerParams(
            collective_id=0, has_side_effects=True, vmem_limit_bytes=60 * 1024 * 1024
        ),
        name="hologram",
    )(target, band_mask, depth_index, turn, small, matrices, flat, short)


def solution(mesh):
    in_specs = (P("depth", None, "rows", None), P("depth"), P("depth", None, None))
    out_specs = P(None, ("depth", "rows"), None)
    return jax.shard_map(local, mesh=mesh, in_specs=in_specs, out_specs=out_specs, check_vma=False)
```

```python
import functools
import math

import jax
import jax.numpy as jnp
import ml_dtypes
import numpy as np
from jax import lax
from jax.experimental import pallas as pl
from jax.experimental.pallas import tpu as pltpu
from jax.sharding import PartitionSpec as P

MESH = pl.DeviceIdType.MESH
N = 4096
LOW = 32
HIGH = 128
Z = 8
TILES = 16
WIDE = 6
SINGLE = 4
CHUNKS = WIDE + SINGLE
ALONE = 2 * WIDE
PAIRED = (0, 8, 15)
FAR = (4, 3, 5, 2, 6, 1, 7)
F32 = jnp.float32
BF16 = jnp.bfloat16


def tables():
    angle = 2.0 * np.pi / N * np.outer(np.arange(LOW), np.arange(HIGH))
    turn = np.stack([np.cos(angle), np.sin(angle)]) / 64.0
    turn = np.broadcast_to(turn[:, :, None, :], (2, LOW, 8, HIGH)).astype(np.float32)
    angle = 2.0 * np.pi / LOW * np.outer(np.arange(1, 4), np.arange(8))
    small = np.stack([np.cos(angle), np.sin(angle)])
    small = np.broadcast_to(small[:, :, :, None, None], (2, 3, 8, 8, HIGH)).astype(np.float32)
    angle = 2.0 * np.pi / HIGH * (np.outer(np.arange(HIGH), np.arange(HIGH)) % HIGH)
    cosine, sine = np.cos(angle), np.sin(angle)
    ahead = np.block([[cosine, -sine], [sine, cosine]])
    parts = []
    for matrix in (ahead, ahead.T):
        top = matrix.astype(np.float32).astype(ml_dtypes.bfloat16)
        rest = (matrix - top.astype(np.float64)).astype(np.float32).astype(ml_dtypes.bfloat16)
        parts += [top, rest]
    order = np.arange(256).reshape(2, 2, 64).swapaxes(0, 1).reshape(256)
    parts += [parts[2][order], parts[3][order]]
    angle = 2.0 * np.pi / LOW * np.outer(np.arange(LOW), np.arange(LOW))
    cosine, sine = np.cos(angle), np.sin(angle)
    short = np.block([[cosine, -sine], [sine, cosine]])
    short = short.reshape(2, Z, 4, 2 * LOW).swapaxes(0, 1).reshape(2 * LOW, 2 * LOW)
    top = short.astype(np.float32).astype(ml_dtypes.bfloat16)
    rest = (short - top.astype(np.float64)).astype(np.float32).astype(ml_dtypes.bfloat16)
    return turn, small, np.stack(parts), turn[:, :, 0, :].copy(), np.stack([top, rest])


def dft4(a, sign):
    (r0, i0), (r1, i1), (r2, i2), (r3, i3) = a
    s0r, s0i, d0r, d0i = r0 + r2, i0 + i2, r0 - r2, i0 - i2
    s1r, s1i, d1r, d1i = r1 + r3, i1 + i3, r1 - r3, i1 - i3
    up, down = (d0r - d1i, d0i + d1r), (d0r + d1i, d0i - d1r)
    first, third = (up, down) if sign > 0 else (down, up)
    return [(s0r + s1r, s0i + s1i), first, (s0r - s1r, s0i - s1i), third]


def turned4(columns, small_ref, part, sign):
    turned = dft4(columns, sign)
    for k in range(1, 4):
        r, i = turned[k]
        c, s = small_ref[0, k - 1, part], small_ref[1, k - 1, part]
        turned[k] = (r * c + i * s, i * c - r * s) if sign < 0 else (r * c - i * s, i * c + r * s)
    return turned


def dft8(rows, sign):
    half = math.sqrt(0.5)
    even = dft4(rows[0::2], sign)
    odd = dft4(rows[1::2], sign)
    (r1, i1), (r2, i2), (r3, i3) = odd[1:]
    if sign < 0:
        odd = [odd[0], ((r1 + i1) * half, (i1 - r1) * half), (i2, -r2), ((i3 - r3) * half, (-r3 - i3) * half)]
    else:
        odd = [odd[0], ((r1 - i1) * half, (i1 + r1) * half), (-i2, r2), ((-r3 - i3) * half, (r3 - i3) * half)]
    result = [(e[0] + o[0], e[1] + o[1]) for e, o in zip(even, odd)]
    return result + [(e[0] - o[0], e[1] - o[1]) for e, o in zip(even, odd)]


def dft32(re, im, small_ref, sign):
    columns = [(re[8 * n : 8 * n + 8], im[8 * n : 8 * n + 8]) for n in range(4)]
    turned = turned4(columns, small_ref, slice(None), sign)
    re = jnp.stack([t[0] for t in turned])
    im = jnp.stack([t[1] for t in turned])
    return dft8([(re[:, n], im[:, n]) for n in range(8)], sign)


def joined(pieces):
    return jnp.concatenate([p[0] for p in pieces]), jnp.concatenate([p[1] for p in pieces])


def split_dot(left, w_ref, which, rows=slice(None)):
    top = left.astype(BF16)
    rest = (left - top.astype(F32)).astype(BF16)
    w_top, w_rest = w_ref[which, rows], w_ref[which + 1, rows]
    dot = functools.partial(jnp.dot, preferred_element_type=F32)
    return dot(top, w_top) + (dot(rest, w_top) + dot(top, w_rest))


def along_lanes(re, im, w_ref, which):
    left = jnp.concatenate([re.reshape(8 * LOW, HIGH), im.reshape(8 * LOW, HIGH)], axis=1)
    result = split_dot(left, w_ref, which)
    return result[:, :HIGH].reshape(LOW, 8, HIGH), result[:, HIGH:].reshape(LOW, 8, HIGH)


def kernel(
    x_ref, mask_ref, level_ref, turn_ref, small_ref, w_ref, flat_ref, short_ref, out_ref,
    xbuf, tbuf, send, recv, prop, part, ring, own, pair, final, final_in, mask_in, level_at, level_out, level_in,
    turn, small, w, flat, short, z_out, z_in, par_out, par_in, sum_out, sum_in, mate_in, mate_own, stage,
    x_sem, in_sem, send_sem, recv_sem, ring_send, ring_recv, pair_send, pair_recv, final_send, final_recv,
    par_send, par_recv, z_send, z_recv, all_send, all_recv, sum_send, sum_recv, mate_send, mate_recv,
):
    depth = lax.axis_index("depth")
    row = lax.axis_index("rows")
    z, y_lo = depth // 2, lax.rem(depth, 2)
    core, y_hi, x = lax.rem(row, 2), lax.rem(row // 2, 4), row // 8
    other = depth + 1 - 2 * y_lo
    up, down = lax.rem(depth + 2, 2 * Z), lax.rem(depth + 2 * Z - 2, 2 * Z)

    column = (x * 4 + lax.rem(y_hi + y_lo * core, 4)) * 2 + core
    mate = (x * 4 + lax.rem(y_hi + core * (3 - 2 * y_lo), 4)) * 2 + core

    def place(to_x, to_y, to_core):
        return (to_x * 4 + to_y) * 2 + to_core, (to_x * 4 + lax.rem(to_y + to_core * (1 - y_lo), 4)) * 2 + to_core

    def peer(i):
        h = lax.rem(i, 4)
        to_y = lax.rem(y_hi + lax.rem(h, 2) * 2 + h // 2, 4)
        to_core = lax.rem(core + lax.rem(i // 4, 2), 2)
        to_x = lax.rem(x + i // 8, 4)
        return place(to_x, to_y, to_core)

    xs = [lax.rem(x + k, 4) for k in range(4)]
    ys = [lax.rem(y_hi + y_lo + k, 4) for k in range(4)]
    cores = [core, 1 - core]
    near_first = [place(xs[i], ys[h], c) for i in range(4) for c in cores for h in (1, 2, 0, 3)]
    far_first = [place(xs[i], ys[h], c) for i in (2, 1, 3, 0) for h in (1, 2, 0, 3) for c in cores]

    def load(g):
        rows = pl.ds(pl.multiple_of(g * 32, 32), 32)
        return pltpu.make_async_copy(x_ref.at[0, :, rows, :], xbuf.at[:, rows, :], x_sem.at[g])

    load_small = pltpu.make_async_copy(small_ref, small, in_sem.at[0])
    load_turn = pltpu.make_async_copy(turn_ref, turn, in_sem.at[1])
    load_w = pltpu.make_async_copy(w_ref, w, in_sem.at[2])
    load_level = pltpu.make_async_copy(level_ref, level_at, in_sem.at[3])
    load_small.start()
    load(0).start()
    load_turn.start()
    for g in range(1, 4):
        load(g).start()
    load_w.start()
    load_level.start()
    load_flat = pltpu.make_async_copy(flat_ref, flat, in_sem.at[4])
    load_short = pltpu.make_async_copy(short_ref, short, in_sem.at[5])
    load_flat.start()
    load_short.start()

    barrier = pltpu.get_barrier_semaphore()

    with jax.named_scope("greet"):
        for to in [(other, r) for r, _ in far_first] + [(2 * lax.rem(z + k, Z) + y_lo, row) for k in FAR] + [
            (2 * lax.rem(z + k, Z) + 1 - y_lo, mate) for k in FAR
        ]:
            pl.semaphore_signal(barrier, inc=1, device_id=to, device_id_type=MESH)

    load_small.wait()
    load_turn.wait()

    def width_first(t, c):
        rows = pl.ds(pl.multiple_of(t * 8, 8), 8)
        for m in range(0, 8, 2):
            columns = [
                tuple(jnp.stack([xbuf[k, rows, a * HIGH : (a + 1) * HIGH] for a in (8 * n + m, 8 * n + m + 1)]) for k in range(2))
                for n in range(4)
            ]
            for k, (r, i) in enumerate(turned4(columns, small, slice(m, m + 2), -1)):
                stage[0, m : m + 2, k] = r
                stage[1, m : m + 2, k] = i
        for k in range(0, 4, 2):
            pieces = dft8([(stage[0, n, k : k + 2], stage[1, n, k : k + 2]) for n in range(8)], -1)
            for n in range(8):
                re, im = pieces[n]
                to = slice(4 * n + k, 4 * n + k + 2)
                cosine, sine = turn[0, to], turn[1, to]
                tbuf[to, 0, rows, :] = re * cosine + im * sine
                tbuf[to, 1, rows, :] = im * cosine - re * sine
        return c

    def width_group(g, c):
        load(g).wait()
        return lax.fori_loop(0, 4, lambda t, c: width_first(g * 4 + t, c), c)

    with jax.named_scope("A1"):
        lax.fori_loop(0, 4, width_group, 0)

    load_level.wait()
    level_out[...] = jnp.full((8, HIGH), level_at[0].astype(F32))
    load_w.wait()
    load_flat.wait()
    load_short.wait()
    with jax.named_scope("barrier"):
        pl.semaphore_wait(barrier, 46)
    mask_copy = pltpu.make_async_remote_copy(
        mask_ref, mask_in, par_send.at[0], par_recv.at[0], device_id=(other, row), device_id_type=MESH
    )
    level_copy = pltpu.make_async_remote_copy(
        level_out, level_in, par_send.at[1], par_recv.at[1], device_id=(other, row), device_id_type=MESH
    )
    mask_copy.start()
    level_copy.start()

    def exchange(q, t0, n, to, block):
        tiles = pl.ds(t0, n)
        return pltpu.make_async_remote_copy(
            send.at[tiles, block], recv.at[tiles, row], send_sem, recv_sem.at[q],
            device_id=(other, to), device_id_type=MESH,
        )

    def exchange_whole(q, t0, n):
        tiles = pl.ds(t0, n)
        return pltpu.make_async_remote_copy(
            send.at[tiles], recv.at[tiles], send_sem, recv_sem.at[q],
            device_id=(other, row), device_id_type=MESH,
        )

    def exchange_all(q, t0, n):
        for to, block in near_first if n > 1 else far_first:
            exchange(q, t0, n, to, block).start()

    def along_z(out, into, send_sem, recv_sem, k, shared=False):
        to = lax.rem(z + k, Z)
        return pltpu.make_async_remote_copy(
            out if shared else out.at[to], into.at[z], send_sem, recv_sem,
            device_id=(2 * to + y_lo, row), device_id_type=MESH,
        )

    def amount(buffer, send_sem, recv_sem):
        return pltpu.make_async_remote_copy(
            buffer, buffer, send_sem, recv_sem, device_id=(other, row), device_id_type=MESH
        )

    seven = pl.ds(0, Z - 1)
    all_z = amount(z_in.at[:, seven], z_send, z_recv)
    all_par = amount(par_in.at[seven], all_send, all_recv)
    all_mate = amount(mate_in, mate_send, mate_recv)

    def width_last(g, c):
        @pl.when(g > 0)
        def _():
            for h in range(4):
                exchange(0, 0, 2, *peer((g - 1) * 4 + h)).start()

        for h in range(4):
            _, block = peer(g * 4 + h)
            both = split_dot(jnp.concatenate([tbuf[block, 0], tbuf[block, 1]], axis=1), w, 0)
            for k in range(2):
                send[:, block, k] = both[:, k * HIGH : (k + 1) * HIGH].T.reshape(TILES, 8, HIGH)
        return c

    with jax.named_scope("A2"):
        lax.fori_loop(0, 8, width_last, 0)
    for j in range(SINGLE):
        for g in range(8):
            block = send[ALONE + j, 4 * g : 4 * g + 4].reshape(8, 8, HIGH)
            z_out[j, :, 8 * g : 8 * g + 8, :] = jnp.swapaxes(block, 0, 1)
    lax.fori_loop(28, 32, lambda i, c: (exchange(0, 0, 2, *peer(i)).start(), c)[1], 0)
    def apart(j):
        for k in FAR:
            along_z(z_out.at[j], z_in.at[j], z_send, z_recv, k).start()
        z_in[j, z] = z_out[j, z]

    apart(0)
    apart(1)
    exchange_all(1, 2, 2)

    mask_copy.wait()
    level_copy.wait()
    distance = 100.0 + 2.0 * level_in[...]

    def cutoff(k):
        total = jnp.sum(mask_in[0, k : k + 1, :].astype(F32), axis=1, keepdims=True)
        return jnp.broadcast_to((total + 1.0) * 0.5, (8, HIGH))

    cut_y, cut_x = cutoff(0), cutoff(1)
    line = lax.broadcasted_iota(jnp.int32, (8, HIGH), 0)
    about = jnp.where(line == 0, distance, jnp.where(line == 1, cut_y, cut_x))
    par_out[...] = about
    par_in[z] = about
    shape = (8, 8, HIGH)

    def signed(k):
        return jnp.where(k < N // 2, k, k - N).astype(F32)

    def propagate(t, g, k_x, distance, cut_y, cut_x):
        k_y = signed(lax.broadcasted_iota(jnp.int32, shape, 0) + g * 8 + 32 * lax.broadcasted_iota(jnp.int32, shape, 2))
        f_y, f_x = k_y * (1.0 / N), k_x * (1.0 / N)
        square = f_y * f_y + f_x * f_x
        quarters = (-4.0 * distance[None]) * (square / (2.0 + jnp.sqrt(4.0 - square)))
        whole = jnp.floor(quarters + 0.5)
        v = (quarters - whole) * (0.5 * math.pi)
        quadrant = whole - 4.0 * jnp.floor(whole * 0.25)
        v2 = v * v
        sine = v + v * v2 * (-1.6666654611e-1 + v2 * (8.3321608736e-3 - v2 * 1.9515295891e-4))
        cosine = 1.0 - 0.5 * v2 + v2 * v2 * (4.166664568298827e-2 + v2 * (-1.388731625493765e-3 + v2 * 2.443315711809948e-5))
        odd = (quadrant == 1.0) | (quadrant == 3.0)
        re = jnp.where(odd, sine, cosine)
        im = jnp.where(odd, cosine, sine)
        inside = (jnp.abs(k_y) < cut_y[None]) & (jnp.abs(k_x) < cut_x[None])
        weight = jnp.where(inside, 1.0, 0.0)
        prop[t, pl.ds(g * 8, 8), 0] = jnp.where((quadrant == 1.0) | (quadrant == 2.0), -re, re) * weight
        prop[t, pl.ds(g * 8, 8), 1] = jnp.where(quadrant >= 2.0, -im, im) * weight

    def propagate_tile(i, c):
        t, g = i // 4, lax.rem(i, 4)
        k_x = signed(column + 32 * (t * 8 + lax.broadcasted_iota(jnp.int32, shape, 1)))
        propagate(t, g, k_x, distance, cut_y, cut_x)
        return c

    with jax.named_scope("H"):
        lax.fori_loop(0, 4 * ALONE, propagate_tile, 0)
    for k in FAR:
        along_z(par_out, par_in, all_send, all_recv, k, True).start()

    def prepare_alone():
        all_z.wait_recv()
        all_par.wait_recv()
        for j in range(SINGLE):
            for g in range(8):
                block = jnp.swapaxes(z_in[j, :, 8 * g : 8 * g + 8, :], 0, 1)
                send[ALONE + j, 4 * g : 4 * g + 4] = block.reshape(4, 2, 8, HIGH)
        each = [jnp.concatenate([par_in[p, j : j + 1, :] for p in range(8)]) for j in range(3)]

        def group(i, c):
            t = ALONE + i // 4
            k_x = signed(jnp.full(shape, column + 32 * (8 * t + z), jnp.int32))
            propagate(t, lax.rem(i, 4), k_x, *each)
            return c

        lax.fori_loop(0, 4 * SINGLE, group, 0)

    def height(t, c):
        re, im = joined(dft32(recv[t, :, 0], recv[t, :, 1], small, -1))
        cosine, sine = turn[0], turn[1]
        re, im = along_lanes(re * cosine + im * sine, im * cosine - re * sine, w, 0)
        p_re, p_im = prop[t, :, 0], prop[t, :, 1]
        re, im = along_lanes(re * p_re - im * p_im, re * p_im + im * p_re, w, 2)
        re, im = joined(dft32(re * cosine - im * sine, im * cosine + re * sine, small, 1))
        part[t, :, 0] = re
        part[t, :, 1] = im
        return c

    def to_mate(k):
        to = lax.rem(z + k, Z)
        return pltpu.make_async_remote_copy(
            sum_out.at[SINGLE - 1, to], mate_in.at[z], mate_send, mate_recv,
            device_id=(2 * to + 1 - y_lo, mate), device_id_type=MESH,
        )

    def height_alone(j):
        t = ALONE + j
        re, im = joined(dft32(recv[t, :, 0], recv[t, :, 1], small, -1))
        cosine, sine = turn[0], turn[1]
        re, im = along_lanes(re * cosine + im * sine, im * cosine - re * sine, w, 0)
        p_re, p_im = prop[t, :, 0], prop[t, :, 1]
        left = jnp.concatenate(
            [jnp.sum(re * p_re - im * p_im, axis=1), jnp.sum(re * p_im + im * p_re, axis=1)], axis=1
        )
        both = split_dot(left, w, 2)
        re, im = both[:, :HIGH], both[:, HIGH:]
        cosine, sine = flat[0], flat[1]
        right = jnp.concatenate([re * cosine - im * sine, im * cosine + re * sine])
        top = right.astype(BF16)
        rest = (right - top.astype(F32)).astype(BF16)
        dot = functools.partial(jnp.dot, preferred_element_type=F32)
        result = dot(short[0], top) + (dot(short[0], rest) + dot(short[1], top))
        sum_out[j] = result.reshape(Z, 8, HIGH)
        sum_in[j, z] = sum_out[j, z]
        if j == SINGLE - 1:
            for k in FAR + (0,):
                to_mate(k).start()
        for k in FAR:
            along_z(sum_out.at[j], sum_in.at[j], sum_send, sum_recv.at[j], k).start()

    def ring_copy(q, t0, n, step, source):
        tiles = pl.ds(t0, n)
        return pltpu.make_async_remote_copy(
            part.at[tiles, pl.ds(source * 4, 4)], ring.at[tiles, step], ring_send,
            ring_recv.at[q, {4: 0, 5: 1, 6: 3}.get(step, step)],
            device_id=(up if step < 4 else down, row), device_id_type=MESH,
        )

    def ring_wait(q, t0, n, step):
        blocks = ring.at[pl.ds(t0, n), pl.ds(0, 1 if step == 2 else 2)]
        amount(blocks, ring_send, ring_recv.at[q, step]).wait_recv()

    def ring_step(q, t0, n, step):
        tiles = pl.ds(t0, n)
        lines = [(step, lax.rem(z + 4 - step, Z))] + ([(step + 4, lax.rem(z + 5 + step, Z))] if step < 3 else [])
        if step > 0:
            ring_wait(q, t0, n, step - 1)
        for i, source in lines:
            if step > 0:
                block = pl.ds(source * 4, 4)
                part[tiles, block] = part[tiles, block] + ring[tiles, i - 1]
        for i, source in lines:
            ring_copy(q, t0, n, i, source).start()

    def pair_copy(q):
        tiles = pl.ds(PAIRED[q], PAIRED[q + 1] - PAIRED[q])
        return pltpu.make_async_remote_copy(
            own.at[tiles, pl.ds(y_lo * 2, 2)], pair.at[tiles], pair_send.at[q], pair_recv.at[q],
            device_id=(other, mate), device_id_type=MESH,
        )

    def ring_end(q, t0, n):
        tiles = pl.ds(t0, n)
        ring_wait(q, t0, n, 3)
        own[tiles] = part[tiles, pl.ds(z * 4, 4)] + (ring[tiles, 3] + ring[tiles, 6])

    def chunk(q, t0, n, ahead, before=None, ended=None):
        with jax.named_scope("wait_a2a"):
            exchange_whole(q, t0, n).wait_recv()
        with jax.named_scope("C"):
            lax.fori_loop(t0, t0 + n, height, 0)
        ring_step(q, t0, n, 0)
        ahead()
        if before is not None:
            ring_step(*before, 2)
        if ended is not None:
            ring_end(*ended)
        with jax.named_scope("ring"):
            ring_step(q, t0, n, 1)
            if before is not None:
                ring_step(*before, 3)

    keep = 2 - 2 * y_lo

    def deliver(half, to):
        return pltpu.make_async_remote_copy(
            final.at[half, to], final_in.at[half, column], final_send, final_recv.at[half],
            device_id=(other, to), device_id_type=MESH,
        )

    def deliver_whole(half):
        return pltpu.make_async_remote_copy(
            final.at[half], final_in.at[half], final_send, final_recv.at[half],
            device_id=(other, row), device_id_type=MESH,
        )

    def hand_over(half):
        tiles = pl.ds(half * 8, 8)
        for a in range(2):
            block = [(own[tiles, keep + a, k] + pair[tiles, a, k]).reshape(64, HIGH) for k in range(2)]
            final[half, a * 16 : a * 16 + 16] = jnp.concatenate(block).T.reshape(16, 8, HIGH)

    def dispatch(half):
        for to, _ in far_first:
            deliver(half, to).start()

    chunk(0, 0, 2, lambda: exchange_all(2, 4, 2))

    def second():
        exchange_all(3, 6, 2)
        apart(2)
        apart(3)

    chunk(1, 2, 2, second, (0, 0, 2))

    def middle(q, c):
        def ahead():
            @pl.when(q < WIDE - 2)
            def _():
                exchange_all(q + 2, 2 * q + 4, 2)

            @pl.when(q >= WIDE - 2)
            def _():
                for j in range(2):
                    i = 2 * (q + 2 - WIDE) + j
                    exchange_all(WIDE + i, ALONE + i, 1)

            @pl.when(q == 3)
            def _():
                prepare_alone()

        chunk(q, 2 * q, 2, ahead, (q - 1, 2 * q - 2, 2), (q - 2, 2 * q - 4, 2))
        return c

    lax.fori_loop(2, WIDE, middle, 0)
    def single(j):
        with jax.named_scope("wait_alone"):
            exchange_whole(WIDE + j, ALONE + j, 1).wait_recv()
        if j == SINGLE - 2:
            pair_copy(0).start()
        with jax.named_scope("C_alone"):
            height_alone(j)

    def summed(j):
        amount(sum_in.at[j, seven], sum_send, sum_recv.at[j]).wait_recv()
        lines = jnp.swapaxes(sum_in[j], 0, 1)
        for k in range(2):
            own[ALONE + j, :, k] = lines[4 * k : 4 * k + 4]

    single(0)
    with jax.named_scope("ring2"):
        ring_end(WIDE - 2, ALONE - 4, 2)
        ring_step(WIDE - 1, ALONE - 2, 2, 2)
    single(1)
    with jax.named_scope("ring3"):
        ring_step(WIDE - 1, ALONE - 2, 2, 3)
        summed(0)
    single(2)
    with jax.named_scope("ring_end"):
        ring_end(WIDE - 1, ALONE - 2, 2)
        summed(1)
    single(3)
    with jax.named_scope("pair0"):
        summed(2)
        pair_copy(1).start()
        pair_copy(0).wait_recv()
        hand_over(0)
    with jax.named_scope("dispatch0"):
        dispatch(0)
    with jax.named_scope("sums"):
        summed(SINGLE - 1)
        all_mate.wait_recv()
        lines = jnp.swapaxes(mate_in[...], 0, 1)
        for k in range(2):
            mate_own[:, k] = lines[4 * k : 4 * k + 4]
        pair[TILES - 1] = mate_own[pl.ds(keep, 2)]
    with jax.named_scope("pair1"):
        pair_copy(1).wait_recv()
    with jax.named_scope("pack1"):
        hand_over(1)
    with jax.named_scope("dispatch1"):
        dispatch(1)

    amount(send, send_sem, recv_sem.at[0]).wait_send()
    amount(ring, ring_send, ring_recv.at[0, 0]).wait_send()
    for q in range(2):
        pair_copy(q).wait_send()
    all_z.wait_send()
    all_par.wait_send()
    all_mate.wait_send()
    amount(sum_in.at[:, seven], sum_send, sum_recv.at[0]).wait_send()
    with jax.named_scope('final_wait0'):
        deliver_whole(0).wait_recv()
    both = split_dot(final_in[0].reshape(8 * LOW, HIGH), w, 4, slice(0, HIGH))
    with jax.named_scope("final_wait"):
        deliver_whole(1).wait_recv()
    both = both + split_dot(final_in[1].reshape(8 * LOW, HIGH), w, 4, slice(HIGH, 2 * HIGH))
    re, im = both[:, :HIGH].reshape(LOW, 8, HIGH), both[:, HIGH:].reshape(LOW, 8, HIGH)
    cosine, sine = turn[0] * 0.25, turn[1] * 0.25
    pieces = dft32(re * cosine - im * sine, im * cosine + re * sine, small, 1)
    for k in range(8):
        for j in range(4):
            lanes = pl.ds((k * 4 + j) * HIGH, HIGH)
            out_ref[0, :, lanes] = pieces[k][0][j]
            out_ref[1, :, lanes] = pieces[k][1][j]
    with jax.named_scope("last_sends"):
        amount(final, final_send, final_recv.at[0]).wait_send()


def local(target, depth_index, band_mask):
    turn, small, matrices, flat, short = tables()
    anywhere = pl.BlockSpec(memory_space=pl.ANY)
    dma = pltpu.SemaphoreType.DMA
    return pl.pallas_call(
        kernel,
        out_shape=pltpu.VMEM((2, 8, N), F32),
        in_specs=[anywhere] * 2 + [pl.BlockSpec(memory_space=pltpu.HBM)] + [anywhere] * 5,
        out_specs=pl.BlockSpec(memory_space=pltpu.VMEM),
        scratch_shapes=[
            pltpu.VMEM((2, HIGH, N), F32),
            pltpu.VMEM((LOW, 2, HIGH, HIGH), F32),
            pltpu.VMEM((TILES, LOW, 2, 8, HIGH), F32),
            pltpu.VMEM((TILES, LOW, 2, 8, HIGH), F32),
            pltpu.VMEM((TILES, LOW, 2, 8, HIGH), F32),
            pltpu.VMEM((TILES, LOW, 2, 8, HIGH), F32),
            pltpu.VMEM((ALONE, 7, 4, 2, 8, HIGH), F32),
            pltpu.VMEM((TILES, 4, 2, 8, HIGH), F32),
            pltpu.VMEM((TILES, 2, 2, 8, HIGH), F32),
            pltpu.VMEM((2, LOW, 8, HIGH), F32),
            pltpu.VMEM((2, LOW, 8, HIGH), F32),
            pltpu.VMEM((1, 2, N), jnp.int32),
            pltpu.SMEM((1,), jnp.int32),
            pltpu.VMEM((8, HIGH), F32),
            pltpu.VMEM((8, HIGH), F32),
            pltpu.VMEM(turn.shape, F32),
            pltpu.VMEM(small.shape, F32),
            pltpu.VMEM(matrices.shape, BF16),
            pltpu.VMEM(flat.shape, F32),
            pltpu.VMEM(short.shape, BF16),
            pltpu.VMEM((SINGLE, Z, 2 * LOW, HIGH), F32),
            pltpu.VMEM((SINGLE, Z, 2 * LOW, HIGH), F32),
            pltpu.VMEM((8, HIGH), F32),
            pltpu.VMEM((Z, 8, HIGH), F32),
            pltpu.VMEM((SINGLE, Z, 8, HIGH), F32),
            pltpu.VMEM((SINGLE, Z, 8, HIGH), F32),
            pltpu.VMEM((Z, 8, HIGH), F32),
            pltpu.VMEM((4, 2, 8, HIGH), F32),
            pltpu.VMEM((2, 8, 4, 8, HIGH), F32),
            dma((4,)),
            dma((6,)),
            dma,
            dma((CHUNKS,)),
            dma,
            dma((WIDE, 4)),
            dma((2,)),
            dma((2,)),
            dma,
            dma((2,)),
            dma((2,)),
            dma((2,)),
            dma,
            dma,
            dma,
            dma,
            dma,
            dma((SINGLE,)),
            dma,
            dma,
        ],
        compiler_params=pltpu.CompilerParams(
            collective_id=0, has_side_effects=True, vmem_limit_bytes=60 * 1024 * 1024
        ),
        name="hologram",
    )(target, band_mask, depth_index, turn, small, matrices, flat, short)


def solution(mesh):
    in_specs = (P("depth", None, "rows", None), P("depth"), P("depth", None, None))
    out_specs = P(None, ("depth", "rows"), None)
    return jax.shard_map(local, mesh=mesh, in_specs=in_specs, out_specs=out_specs, check_vma=False)
```

```python
import functools
import math

import jax
import jax.numpy as jnp
import ml_dtypes
import numpy as np
from jax import lax
from jax.experimental import pallas as pl
from jax.experimental.pallas import tpu as pltpu
from jax.sharding import PartitionSpec as P

MESH = pl.DeviceIdType.MESH
N = 4096
LOW = 32
HIGH = 128
Z = 8
TILES = 16
WIDE = 6
SINGLE = 4
CHUNKS = WIDE + SINGLE
ALONE = 2 * WIDE
PAIRED = (0, 8, 15)
FAR = (4, 3, 5, 2, 6, 1, 7)
F32 = jnp.float32
BF16 = jnp.bfloat16


def tables():
    angle = 2.0 * np.pi / N * np.outer(np.arange(LOW), np.arange(HIGH))
    turn = np.stack([np.cos(angle), np.sin(angle)]) / 64.0
    turn = np.broadcast_to(turn[:, :, None, :], (2, LOW, 8, HIGH)).astype(np.float32)
    angle = 2.0 * np.pi / LOW * np.outer(np.arange(1, 4), np.arange(8))
    small = np.stack([np.cos(angle), np.sin(angle)])
    small = np.broadcast_to(small[:, :, :, None, None], (2, 3, 8, 8, HIGH)).astype(np.float32)
    angle = 2.0 * np.pi / HIGH * (np.outer(np.arange(HIGH), np.arange(HIGH)) % HIGH)
    cosine, sine = np.cos(angle), np.sin(angle)
    ahead = np.block([[cosine, -sine], [sine, cosine]])
    parts = []
    for matrix in (ahead, ahead.T):
        top = matrix.astype(np.float32).astype(ml_dtypes.bfloat16)
        rest = (matrix - top.astype(np.float64)).astype(np.float32).astype(ml_dtypes.bfloat16)
        parts += [top, rest]
    order = np.arange(256).reshape(2, 2, 64).swapaxes(0, 1).reshape(256)
    parts += [parts[2][order], parts[3][order]]
    angle = 2.0 * np.pi / LOW * np.outer(np.arange(LOW), np.arange(LOW))
    cosine, sine = np.cos(angle), np.sin(angle)
    short = np.block([[cosine, -sine], [sine, cosine]])
    short = short.reshape(2, Z, 4, 2 * LOW).swapaxes(0, 1).reshape(2 * LOW, 2 * LOW)
    top = short.astype(np.float32).astype(ml_dtypes.bfloat16)
    rest = (short - top.astype(np.float64)).astype(np.float32).astype(ml_dtypes.bfloat16)
    return turn, small, np.stack(parts), turn[:, :, 0, :].copy(), np.stack([top, rest])


def dft4(a, sign):
    (r0, i0), (r1, i1), (r2, i2), (r3, i3) = a
    s0r, s0i, d0r, d0i = r0 + r2, i0 + i2, r0 - r2, i0 - i2
    s1r, s1i, d1r, d1i = r1 + r3, i1 + i3, r1 - r3, i1 - i3
    up, down = (d0r - d1i, d0i + d1r), (d0r + d1i, d0i - d1r)
    first, third = (up, down) if sign > 0 else (down, up)
    return [(s0r + s1r, s0i + s1i), first, (s0r - s1r, s0i - s1i), third]


def turned4(columns, small_ref, part, sign):
    turned = dft4(columns, sign)
    for k in range(1, 4):
        r, i = turned[k]
        c, s = small_ref[0, k - 1, part], small_ref[1, k - 1, part]
        turned[k] = (r * c + i * s, i * c - r * s) if sign < 0 else (r * c - i * s, i * c + r * s)
    return turned


def dft8(rows, sign):
    half = math.sqrt(0.5)
    even = dft4(rows[0::2], sign)
    odd = dft4(rows[1::2], sign)
    (r1, i1), (r2, i2), (r3, i3) = odd[1:]
    if sign < 0:
        odd = [odd[0], ((r1 + i1) * half, (i1 - r1) * half), (i2, -r2), ((i3 - r3) * half, (-r3 - i3) * half)]
    else:
        odd = [odd[0], ((r1 - i1) * half, (i1 + r1) * half), (-i2, r2), ((-r3 - i3) * half, (r3 - i3) * half)]
    result = [(e[0] + o[0], e[1] + o[1]) for e, o in zip(even, odd)]
    return result + [(e[0] - o[0], e[1] - o[1]) for e, o in zip(even, odd)]


def dft32(re, im, small_ref, sign):
    columns = [(re[8 * n : 8 * n + 8], im[8 * n : 8 * n + 8]) for n in range(4)]
    turned = turned4(columns, small_ref, slice(None), sign)
    re = jnp.stack([t[0] for t in turned])
    im = jnp.stack([t[1] for t in turned])
    return dft8([(re[:, n], im[:, n]) for n in range(8)], sign)


def joined(pieces):
    return jnp.concatenate([p[0] for p in pieces]), jnp.concatenate([p[1] for p in pieces])


def split_dot(left, w_ref, which, rows=slice(None)):
    top = left.astype(BF16)
    rest = (left - top.astype(F32)).astype(BF16)
    w_top, w_rest = w_ref[which, rows], w_ref[which + 1, rows]
    dot = functools.partial(jnp.dot, preferred_element_type=F32)
    return dot(top, w_top) + (dot(rest, w_top) + dot(top, w_rest))


def along_lanes(re, im, w_ref, which):
    left = jnp.concatenate([re.reshape(8 * LOW, HIGH), im.reshape(8 * LOW, HIGH)], axis=1)
    result = split_dot(left, w_ref, which)
    return result[:, :HIGH].reshape(LOW, 8, HIGH), result[:, HIGH:].reshape(LOW, 8, HIGH)


def kernel(
    x_ref, mask_ref, level_ref, turn_ref, small_ref, w_ref, flat_ref, short_ref, out_ref,
    xbuf, tbuf, send, recv, prop, part, ring, own, pair, final, final_in, mask_in, level_at, level_out, level_in,
    turn, small, w, flat, short, z_out, z_in, par_out, par_in, sum_out, sum_in, mate_in, mate_own, stage,
    x_sem, in_sem, send_sem, recv_sem, ring_send, ring_recv, pair_send, pair_recv, final_send, final_recv,
    par_send, par_recv, z_send, z_recv, all_send, all_recv, sum_send, sum_recv, mate_send, mate_recv,
):
    depth = lax.axis_index("depth")
    row = lax.axis_index("rows")
    z, y_lo = depth // 2, lax.rem(depth, 2)
    core, y_hi, x = lax.rem(row, 2), lax.rem(row // 2, 4), row // 8
    other = depth + 1 - 2 * y_lo
    up, down = lax.rem(depth + 2, 2 * Z), lax.rem(depth + 2 * Z - 2, 2 * Z)

    column = (x * 4 + lax.rem(y_hi + y_lo * core, 4)) * 2 + core
    mate = (x * 4 + lax.rem(y_hi + core * (3 - 2 * y_lo), 4)) * 2 + core

    def place(to_x, to_y, to_core):
        return (to_x * 4 + to_y) * 2 + to_core, (to_x * 4 + lax.rem(to_y + to_core * (1 - y_lo), 4)) * 2 + to_core

    def peer(i):
        h = lax.rem(i, 4)
        to_y = lax.rem(y_hi + lax.rem(h, 2) * 2 + h // 2, 4)
        to_core = lax.rem(core + lax.rem(i // 4, 2), 2)
        to_x = lax.rem(x + i // 8, 4)
        return place(to_x, to_y, to_core)

    xs = [lax.rem(x + k, 4) for k in range(4)]
    ys = [lax.rem(y_hi + y_lo + k, 4) for k in range(4)]
    cores = [core, 1 - core]
    near_first = [place(xs[i], ys[h], c) for i in range(4) for c in cores for h in (1, 2, 0, 3)]
    far_first = [place(xs[i], ys[h], c) for i in (2, 1, 3, 0) for h in (1, 2, 0, 3) for c in cores]

    def load(g):
        rows = pl.ds(pl.multiple_of(g * 32, 32), 32)
        return pltpu.make_async_copy(x_ref.at[0, :, rows, :], xbuf.at[:, rows, :], x_sem.at[g])

    load_small = pltpu.make_async_copy(small_ref, small, in_sem.at[0])
    load_turn = pltpu.make_async_copy(turn_ref, turn, in_sem.at[1])
    load_w = pltpu.make_async_copy(w_ref, w, in_sem.at[2])
    load_level = pltpu.make_async_copy(level_ref, level_at, in_sem.at[3])
    load_small.start()
    load(0).start()
    load_turn.start()
    for g in range(1, 4):
        load(g).start()
    load_w.start()
    load_level.start()
    load_mask = pltpu.make_async_copy(mask_ref, mask_in, in_sem.at[6])
    load_mask.start()
    load_flat = pltpu.make_async_copy(flat_ref, flat, in_sem.at[4])
    load_short = pltpu.make_async_copy(short_ref, short, in_sem.at[5])
    load_flat.start()
    load_short.start()

    barrier = pltpu.get_barrier_semaphore()

    with jax.named_scope("greet"):
        for to in [(other, r) for r, _ in far_first] + [(2 * lax.rem(z + k, Z) + y_lo, row) for k in FAR] + [
            (2 * lax.rem(z + k, Z) + 1 - y_lo, mate) for k in FAR
        ]:
            pl.semaphore_signal(barrier, inc=1, device_id=to, device_id_type=MESH)

    load_small.wait()
    load_turn.wait()

    def width_first(t, c):
        rows = pl.ds(pl.multiple_of(t * 8, 8), 8)
        for m in range(0, 8, 2):
            columns = [
                tuple(jnp.stack([xbuf[k, rows, a * HIGH : (a + 1) * HIGH] for a in (8 * n + m, 8 * n + m + 1)]) for k in range(2))
                for n in range(4)
            ]
            for k, (r, i) in enumerate(turned4(columns, small, slice(m, m + 2), -1)):
                stage[0, m : m + 2, k] = r
                stage[1, m : m + 2, k] = i
        for k in range(0, 4, 2):
            pieces = dft8([(stage[0, n, k : k + 2], stage[1, n, k : k + 2]) for n in range(8)], -1)
            for n in range(8):
                re, im = pieces[n]
                to = slice(4 * n + k, 4 * n + k + 2)
                cosine, sine = turn[0, to], turn[1, to]
                tbuf[to, 0, rows, :] = re * cosine + im * sine
                tbuf[to, 1, rows, :] = im * cosine - re * sine
        return c

    def width_group(g, c):
        load(g).wait()
        return lax.fori_loop(0, 4, lambda t, c: width_first(g * 4 + t, c), c)

    with jax.named_scope("A1"):
        lax.fori_loop(0, 4, width_group, 0)

    load_level.wait()
    load_mask.wait()

    def cutoff(k):
        total = jnp.sum(mask_in[0, k : k + 1, :].astype(F32), axis=1, keepdims=True)
        return jnp.broadcast_to((total + 1.0) * 0.5, (8, HIGH))

    line = lax.broadcasted_iota(jnp.int32, (8, HIGH), 0)
    level = jnp.full((8, HIGH), 100.0 + 2.0 * level_at[0].astype(F32))
    level_out[...] = jnp.where(line == 0, level, jnp.where(line == 1, cutoff(0), cutoff(1)))
    load_w.wait()
    load_flat.wait()
    load_short.wait()
    with jax.named_scope("barrier"):
        pl.semaphore_wait(barrier, 46)
    level_copy = pltpu.make_async_remote_copy(
        level_out, level_in, par_send, par_recv, device_id=(other, row), device_id_type=MESH
    )
    level_copy.start()

    def exchange(q, t0, n, to, block):
        tiles = pl.ds(t0, n)
        return pltpu.make_async_remote_copy(
            send.at[tiles, block], recv.at[tiles, row], send_sem, recv_sem.at[q],
            device_id=(other, to), device_id_type=MESH,
        )

    def exchange_whole(q, t0, n):
        tiles = pl.ds(t0, n)
        return pltpu.make_async_remote_copy(
            send.at[tiles], recv.at[tiles], send_sem, recv_sem.at[q],
            device_id=(other, row), device_id_type=MESH,
        )

    def exchange_all(q, t0, n):
        for to, block in near_first if n > 1 else far_first:
            exchange(q, t0, n, to, block).start()

    def along_z(out, into, send_sem, recv_sem, k, shared=False):
        to = lax.rem(z + k, Z)
        return pltpu.make_async_remote_copy(
            out if shared else out.at[to], into.at[z], send_sem, recv_sem,
            device_id=(2 * to + y_lo, row), device_id_type=MESH,
        )

    def amount(buffer, send_sem, recv_sem):
        return pltpu.make_async_remote_copy(
            buffer, buffer, send_sem, recv_sem, device_id=(other, row), device_id_type=MESH
        )

    seven = pl.ds(0, Z - 1)
    all_z = amount(z_in.at[:, seven], z_send, z_recv)
    all_par = amount(par_in.at[seven], all_send, all_recv)
    all_mate = amount(mate_in, mate_send, mate_recv)

    def width_last(g, c):
        @pl.when(g > 0)
        def _():
            for h in range(4):
                exchange(0, 0, 2, *peer((g - 1) * 4 + h)).start()

        for h in range(4):
            _, block = peer(g * 4 + h)
            both = split_dot(jnp.concatenate([tbuf[block, 0], tbuf[block, 1]], axis=1), w, 0)
            for k in range(2):
                send[:, block, k] = both[:, k * HIGH : (k + 1) * HIGH].T.reshape(TILES, 8, HIGH)
        return c

    with jax.named_scope("A2"):
        lax.fori_loop(0, 8, width_last, 0)
    for j in range(SINGLE):
        for g in range(8):
            block = send[ALONE + j, 4 * g : 4 * g + 4].reshape(8, 8, HIGH)
            z_out[j, :, 8 * g : 8 * g + 8, :] = jnp.swapaxes(block, 0, 1)
    lax.fori_loop(28, 32, lambda i, c: (exchange(0, 0, 2, *peer(i)).start(), c)[1], 0)
    def apart(j):
        for k in FAR:
            along_z(z_out.at[j], z_in.at[j], z_send, z_recv, k).start()
        z_in[j, z] = z_out[j, z]

    apart(0)
    apart(1)
    exchange_all(1, 2, 2)

    level_copy.wait()
    distance, cut_y, cut_x = [jnp.broadcast_to(level_in[j : j + 1, :], (8, HIGH)) for j in range(3)]
    par_out[...] = level_in[...]
    par_in[z] = level_in[...]
    shape = (8, 8, HIGH)

    def signed(k):
        return jnp.where(k < N // 2, k, k - N).astype(F32)

    def propagate(t, g, k_x, distance, cut_y, cut_x):
        k_y = signed(lax.broadcasted_iota(jnp.int32, shape, 0) + g * 8 + 32 * lax.broadcasted_iota(jnp.int32, shape, 2))
        f_y, f_x = k_y * (1.0 / N), k_x * (1.0 / N)
        square = f_y * f_y + f_x * f_x
        quarters = (-4.0 * distance[None]) * (square / (2.0 + jnp.sqrt(4.0 - square)))
        whole = jnp.floor(quarters + 0.5)
        v = (quarters - whole) * (0.5 * math.pi)
        quadrant = whole - 4.0 * jnp.floor(whole * 0.25)
        v2 = v * v
        sine = v + v * v2 * (-1.6666654611e-1 + v2 * (8.3321608736e-3 - v2 * 1.9515295891e-4))
        cosine = 1.0 - 0.5 * v2 + v2 * v2 * (4.166664568298827e-2 + v2 * (-1.388731625493765e-3 + v2 * 2.443315711809948e-5))
        odd = (quadrant == 1.0) | (quadrant == 3.0)
        re = jnp.where(odd, sine, cosine)
        im = jnp.where(odd, cosine, sine)
        inside = (jnp.abs(k_y) < cut_y[None]) & (jnp.abs(k_x) < cut_x[None])
        weight = jnp.where(inside, 1.0, 0.0)
        prop[t, pl.ds(g * 8, 8), 0] = jnp.where((quadrant == 1.0) | (quadrant == 2.0), -re, re) * weight
        prop[t, pl.ds(g * 8, 8), 1] = jnp.where(quadrant >= 2.0, -im, im) * weight

    def propagate_tile(i, c):
        t, g = i // 4, lax.rem(i, 4)
        k_x = signed(column + 32 * (t * 8 + lax.broadcasted_iota(jnp.int32, shape, 1)))
        propagate(t, g, k_x, distance, cut_y, cut_x)
        return c

    with jax.named_scope("H"):
        lax.fori_loop(0, 4 * ALONE, propagate_tile, 0)
    for k in FAR:
        along_z(par_out, par_in, all_send, all_recv, k, True).start()

    def prepare_alone():
        all_z.wait_recv()
        all_par.wait_recv()
        for j in range(SINGLE):
            for g in range(8):
                block = jnp.swapaxes(z_in[j, :, 8 * g : 8 * g + 8, :], 0, 1)
                send[ALONE + j, 4 * g : 4 * g + 4] = block.reshape(4, 2, 8, HIGH)
        each = [jnp.concatenate([par_in[p, j : j + 1, :] for p in range(8)]) for j in range(3)]

        def group(i, c):
            t = ALONE + i // 4
            k_x = signed(jnp.full(shape, column + 32 * (8 * t + z), jnp.int32))
            propagate(t, lax.rem(i, 4), k_x, *each)
            return c

        lax.fori_loop(0, 4 * SINGLE, group, 0)

    def height(t, c):
        re, im = joined(dft32(recv[t, :, 0], recv[t, :, 1], small, -1))
        cosine, sine = turn[0], turn[1]
        re, im = along_lanes(re * cosine + im * sine, im * cosine - re * sine, w, 0)
        p_re, p_im = prop[t, :, 0], prop[t, :, 1]
        re, im = along_lanes(re * p_re - im * p_im, re * p_im + im * p_re, w, 2)
        re, im = joined(dft32(re * cosine - im * sine, im * cosine + re * sine, small, 1))
        part[t, :, 0] = re
        part[t, :, 1] = im
        return c

    def to_mate(k):
        to = lax.rem(z + k, Z)
        return pltpu.make_async_remote_copy(
            sum_out.at[SINGLE - 1, to], mate_in.at[z], mate_send, mate_recv,
            device_id=(2 * to + 1 - y_lo, mate), device_id_type=MESH,
        )

    def height_alone(j):
        t = ALONE + j
        re, im = joined(dft32(recv[t, :, 0], recv[t, :, 1], small, -1))
        cosine, sine = turn[0], turn[1]
        re, im = along_lanes(re * cosine + im * sine, im * cosine - re * sine, w, 0)
        p_re, p_im = prop[t, :, 0], prop[t, :, 1]
        left = jnp.concatenate(
            [jnp.sum(re * p_re - im * p_im, axis=1), jnp.sum(re * p_im + im * p_re, axis=1)], axis=1
        )
        both = split_dot(left, w, 2)
        re, im = both[:, :HIGH], both[:, HIGH:]
        cosine, sine = flat[0], flat[1]
        right = jnp.concatenate([re * cosine - im * sine, im * cosine + re * sine])
        top = right.astype(BF16)
        rest = (right - top.astype(F32)).astype(BF16)
        dot = functools.partial(jnp.dot, preferred_element_type=F32)
        result = dot(short[0], top) + (dot(short[0], rest) + dot(short[1], top))
        sum_out[j] = result.reshape(Z, 8, HIGH)
        sum_in[j, z] = sum_out[j, z]
        if j == SINGLE - 1:
            for k in FAR + (0,):
                to_mate(k).start()
        for k in FAR:
            along_z(sum_out.at[j], sum_in.at[j], sum_send, sum_recv.at[j], k).start()

    def ring_copy(q, t0, n, step, source):
        tiles = pl.ds(t0, n)
        return pltpu.make_async_remote_copy(
            part.at[tiles, pl.ds(source * 4, 4)], ring.at[tiles, step], ring_send,
            ring_recv.at[q, {4: 0, 5: 1, 6: 3}.get(step, step)],
            device_id=(up if step < 4 else down, row), device_id_type=MESH,
        )

    def ring_wait(q, t0, n, step):
        blocks = ring.at[pl.ds(t0, n), pl.ds(0, 1 if step == 2 else 2)]
        amount(blocks, ring_send, ring_recv.at[q, step]).wait_recv()

    def ring_step(q, t0, n, step):
        tiles = pl.ds(t0, n)
        lines = [(step, lax.rem(z + 4 - step, Z))] + ([(step + 4, lax.rem(z + 5 + step, Z))] if step < 3 else [])
        if step > 0:
            ring_wait(q, t0, n, step - 1)
        for i, source in lines:
            if step > 0:
                block = pl.ds(source * 4, 4)
                part[tiles, block] = part[tiles, block] + ring[tiles, i - 1]
        for i, source in lines:
            ring_copy(q, t0, n, i, source).start()

    def pair_copy(q):
        tiles = pl.ds(PAIRED[q], PAIRED[q + 1] - PAIRED[q])
        return pltpu.make_async_remote_copy(
            own.at[tiles, pl.ds(y_lo * 2, 2)], pair.at[tiles], pair_send.at[q], pair_recv.at[q],
            device_id=(other, mate), device_id_type=MESH,
        )

    def ring_end(q, t0, n):
        tiles = pl.ds(t0, n)
        ring_wait(q, t0, n, 3)
        own[tiles] = part[tiles, pl.ds(z * 4, 4)] + (ring[tiles, 3] + ring[tiles, 6])

    def chunk(q, t0, n, ahead, before=None, ended=None):
        with jax.named_scope("wait_a2a"):
            exchange_whole(q, t0, n).wait_recv()
        with jax.named_scope("C"):
            lax.fori_loop(t0, t0 + n, height, 0)
        ring_step(q, t0, n, 0)
        ahead()
        if before is not None:
            ring_step(*before, 2)
        if ended is not None:
            ring_end(*ended)
        with jax.named_scope("ring"):
            ring_step(q, t0, n, 1)
            if before is not None:
                ring_step(*before, 3)

    keep = 2 - 2 * y_lo

    def deliver(half, to):
        return pltpu.make_async_remote_copy(
            final.at[half, to], final_in.at[half, column], final_send, final_recv.at[half],
            device_id=(other, to), device_id_type=MESH,
        )

    def deliver_whole(half):
        return pltpu.make_async_remote_copy(
            final.at[half], final_in.at[half], final_send, final_recv.at[half],
            device_id=(other, row), device_id_type=MESH,
        )

    def hand_over(half):
        tiles = pl.ds(half * 8, 8)
        for a in range(2):
            block = [(own[tiles, keep + a, k] + pair[tiles, a, k]).reshape(64, HIGH) for k in range(2)]
            final[half, a * 16 : a * 16 + 16] = jnp.concatenate(block).T.reshape(16, 8, HIGH)

    def dispatch(half):
        for to, _ in far_first:
            deliver(half, to).start()

    chunk(0, 0, 2, lambda: exchange_all(2, 4, 2))

    def second():
        exchange_all(3, 6, 2)
        apart(2)
        apart(3)

    chunk(1, 2, 2, second, (0, 0, 2))

    def middle(q, c):
        def ahead():
            @pl.when(q < WIDE - 2)
            def _():
                exchange_all(q + 2, 2 * q + 4, 2)

            @pl.when(q >= WIDE - 2)
            def _():
                for j in range(2):
                    i = 2 * (q + 2 - WIDE) + j
                    exchange_all(WIDE + i, ALONE + i, 1)

            @pl.when(q == 3)
            def _():
                prepare_alone()

        chunk(q, 2 * q, 2, ahead, (q - 1, 2 * q - 2, 2), (q - 2, 2 * q - 4, 2))
        return c

    lax.fori_loop(2, WIDE, middle, 0)
    def single(j):
        with jax.named_scope("wait_alone"):
            exchange_whole(WIDE + j, ALONE + j, 1).wait_recv()
        if j == SINGLE - 2:
            pair_copy(0).start()
        with jax.named_scope("C_alone"):
            height_alone(j)

    def summed(j):
        amount(sum_in.at[j, seven], sum_send, sum_recv.at[j]).wait_recv()
        lines = jnp.swapaxes(sum_in[j], 0, 1)
        for k in range(2):
            own[ALONE + j, :, k] = lines[4 * k : 4 * k + 4]

    single(0)
    with jax.named_scope("ring2"):
        ring_end(WIDE - 2, ALONE - 4, 2)
        ring_step(WIDE - 1, ALONE - 2, 2, 2)
    single(1)
    with jax.named_scope("ring3"):
        ring_step(WIDE - 1, ALONE - 2, 2, 3)
        summed(0)
    single(2)
    with jax.named_scope("ring_end"):
        ring_end(WIDE - 1, ALONE - 2, 2)
        summed(1)
    single(3)
    with jax.named_scope("pair0"):
        summed(2)
        pair_copy(1).start()
        pair_copy(0).wait_recv()
        hand_over(0)
    with jax.named_scope("dispatch0"):
        dispatch(0)
    with jax.named_scope("sums"):
        summed(SINGLE - 1)
        all_mate.wait_recv()
        lines = jnp.swapaxes(mate_in[...], 0, 1)
        for k in range(2):
            mate_own[:, k] = lines[4 * k : 4 * k + 4]
        pair[TILES - 1] = mate_own[pl.ds(keep, 2)]
    with jax.named_scope("pair1"):
        pair_copy(1).wait_recv()
    with jax.named_scope("pack1"):
        hand_over(1)
    with jax.named_scope("dispatch1"):
        dispatch(1)

    amount(send, send_sem, recv_sem.at[0]).wait_send()
    amount(ring, ring_send, ring_recv.at[0, 0]).wait_send()
    for q in range(2):
        pair_copy(q).wait_send()
    all_z.wait_send()
    all_par.wait_send()
    all_mate.wait_send()
    amount(sum_in.at[:, seven], sum_send, sum_recv.at[0]).wait_send()
    with jax.named_scope('final_wait0'):
        deliver_whole(0).wait_recv()
    both = split_dot(final_in[0].reshape(8 * LOW, HIGH), w, 4, slice(0, HIGH))
    with jax.named_scope("final_wait"):
        deliver_whole(1).wait_recv()
    both = both + split_dot(final_in[1].reshape(8 * LOW, HIGH), w, 4, slice(HIGH, 2 * HIGH))
    re, im = both[:, :HIGH].reshape(LOW, 8, HIGH), both[:, HIGH:].reshape(LOW, 8, HIGH)
    cosine, sine = turn[0] * 0.25, turn[1] * 0.25
    pieces = dft32(re * cosine - im * sine, im * cosine + re * sine, small, 1)
    for k in range(8):
        for j in range(4):
            lanes = pl.ds((k * 4 + j) * HIGH, HIGH)
            out_ref[0, :, lanes] = pieces[k][0][j]
            out_ref[1, :, lanes] = pieces[k][1][j]
    with jax.named_scope("last_sends"):
        amount(final, final_send, final_recv.at[0]).wait_send()


def local(target, depth_index, band_mask):
    turn, small, matrices, flat, short = tables()
    anywhere = pl.BlockSpec(memory_space=pl.ANY)
    dma = pltpu.SemaphoreType.DMA
    return pl.pallas_call(
        kernel,
        out_shape=pltpu.VMEM((2, 8, N), F32),
        in_specs=[anywhere] * 2 + [pl.BlockSpec(memory_space=pltpu.HBM)] + [anywhere] * 5,
        out_specs=pl.BlockSpec(memory_space=pltpu.VMEM),
        scratch_shapes=[
            pltpu.VMEM((2, HIGH, N), F32),
            pltpu.VMEM((LOW, 2, HIGH, HIGH), F32),
            pltpu.VMEM((TILES, LOW, 2, 8, HIGH), F32),
            pltpu.VMEM((TILES, LOW, 2, 8, HIGH), F32),
            pltpu.VMEM((TILES, LOW, 2, 8, HIGH), F32),
            pltpu.VMEM((TILES, LOW, 2, 8, HIGH), F32),
            pltpu.VMEM((ALONE, 7, 4, 2, 8, HIGH), F32),
            pltpu.VMEM((TILES, 4, 2, 8, HIGH), F32),
            pltpu.VMEM((TILES, 2, 2, 8, HIGH), F32),
            pltpu.VMEM((2, LOW, 8, HIGH), F32),
            pltpu.VMEM((2, LOW, 8, HIGH), F32),
            pltpu.VMEM((1, 2, N), jnp.int32),
            pltpu.SMEM((1,), jnp.int32),
            pltpu.VMEM((8, HIGH), F32),
            pltpu.VMEM((8, HIGH), F32),
            pltpu.VMEM(turn.shape, F32),
            pltpu.VMEM(small.shape, F32),
            pltpu.VMEM(matrices.shape, BF16),
            pltpu.VMEM(flat.shape, F32),
            pltpu.VMEM(short.shape, BF16),
            pltpu.VMEM((SINGLE, Z, 2 * LOW, HIGH), F32),
            pltpu.VMEM((SINGLE, Z, 2 * LOW, HIGH), F32),
            pltpu.VMEM((8, HIGH), F32),
            pltpu.VMEM((Z, 8, HIGH), F32),
            pltpu.VMEM((SINGLE, Z, 8, HIGH), F32),
            pltpu.VMEM((SINGLE, Z, 8, HIGH), F32),
            pltpu.VMEM((Z, 8, HIGH), F32),
            pltpu.VMEM((4, 2, 8, HIGH), F32),
            pltpu.VMEM((2, 8, 4, 8, HIGH), F32),
            dma((4,)),
            dma((7,)),
            dma,
            dma((CHUNKS,)),
            dma,
            dma((WIDE, 4)),
            dma((2,)),
            dma((2,)),
            dma,
            dma((2,)),
            dma,
            dma,
            dma,
            dma,
            dma,
            dma,
            dma,
            dma((SINGLE,)),
            dma,
            dma,
        ],
        compiler_params=pltpu.CompilerParams(
            collective_id=0, has_side_effects=True, vmem_limit_bytes=60 * 1024 * 1024
        ),
        name="hologram",
    )(target, band_mask, depth_index, turn, small, matrices, flat, short)


def solution(mesh):
    in_specs = (P("depth", None, "rows", None), P("depth"), P("depth", None, None))
    out_specs = P(None, ("depth", "rows"), None)
    return jax.shard_map(local, mesh=mesh, in_specs=in_specs, out_specs=out_specs, check_vma=False)
```
